32 devices in a mesh: gx: 4 (over x, core), gy: 8 (over z, y).
Axes of the slice: x: 2, y: 2, z: 4, core: 2. Of those that a mesh axis runs over, the one named last changes fastest.
Arguments:
- node_feats: bfloat16 [40960, 512], P(('gx', 'gy')), may hold values from -6 to 6
- edge_feats: bfloat16 [131072, 512], P(('gx', 'gy')), may hold values from -6 to 6
- senders: int32 [131072], P(('gx', 'gy')), may hold values from 0 to 1791
- receivers: int32 [131072], P(('gx', 'gy')), may hold values from 0 to 1279, as said below
- send_lists: int32 [4096], P(('gx', 'gy')), may hold values from 0 to 1279
- coarse_edges: bfloat16 [5120, 512], P(('gx', 'gy')), may hold values from -6 to 6
- coarse_senders: int32 [5120], P(('gx', 'gy')), may hold values from 0 to 639
- coarse_receivers: int32 [5120], P(('gx', 'gy')), may hold values from 0 to 639, as said below
- edge_w1: bfloat16 [1536, 512], replicated, may hold values from -0.15625 to 0.15625
- edge_b1: float32 [512], replicated, may hold values from -4 to 4
- edge_w2: bfloat16 [512, 512], replicated, may hold values from -0.25 to 0.25
- edge_b2: float32 [512], replicated, may hold values from -3 to 3
- edge_gain: float32 [512], replicated, may hold values from 0.5 to 1.5
- edge_shift: float32 [512], replicated, may hold values from -3 to 3
- node_w1: bfloat16 [1024, 512], replicated, may hold values from -0.1875 to 0.1875
- node_b1: float32 [512], replicated, may hold values from -4 to 4
- node_w2: bfloat16 [512, 512], replicated, may hold values from -0.25 to 0.25
- node_b2: float32 [512], replicated, may hold values from -3 to 3
- node_gain: float32 [512], replicated, may hold values from 0.5 to 1.5
- node_shift: float32 [512], replicated, may hold values from -3 to 3
Outputs:
- new_nodes: bfloat16 [40960, 512], P(('gx', 'gy'))
- new_edges: bfloat16 [131072, 512], P(('gx', 'gy'))
- new_coarse: bfloat16 [5120, 512], P(('gx', 'gy'))
The draws below stay inside these ranges and needn't reach their ends.
Inputs may be any that keep to these rules, and one draw needn't show every extreme that they name: Within one device the receivers start at 0, never fall, and rise by at most one from an edge to the next; within each aligned block of 128 of its edges they span at most 128 nodes. `coarse_receivers`: of the 160 coarse edges of one device, at most 10 have receivers c with the same c // 20.
All inputs are finite; a program needn't handle non-finite values.
Results may differ from the reference program's by a relative error of at most 0.003.
The reference program's roundings to bfloat16 on the way count: a program that leaves them out, or rounds other values in their place, can miss the bound.
Values may be sent and summed in bfloat16 or wider, within the bound.
No kernel may reach another device: no remote copies, remote signals or barrier semaphores. Data moves between devices by JAX's collectives and lax.ppermute only.
A program may use at most 128 MiB of HBM per device.

```python
import jax
import jax.numpy as jnp
from jax import lax

D = 512
N_DEV = 1280
E_DEV = 4096
HB = 128
CE_DEV = 160
NCD = 20
NODES = 40960
EDGES = 131072
NC = 640
CEDGES = 5120
CCAP = 10
N_GX = 4
N_GY = 8


def draw_receivers(key, part):
    groups = EDGES // E_DEV
    blocks = E_DEV // 128
    target = max(0, (N_DEV - 129) * 7 // (8 * (blocks - 1)))

    def one_device(dev_key):
        sub_keys = jax.random.split(dev_key, 3)
        full_block = jax.random.randint(sub_keys[0], (), 0, blocks, dtype=jnp.int32)
        counts = jax.random.randint(sub_keys[1], (blocks,), target // 2, target + target // 2 + 1, dtype=jnp.int32)
        counts = jnp.where(jnp.arange(blocks, dtype=jnp.int32) == full_block, 128, counts)
        coin_draws = jax.random.randint(sub_keys[2], (blocks, 128), 0, 128, dtype=jnp.int32)
        step_flags = (coin_draws < counts[:, None]).astype(jnp.int32).reshape(E_DEV)
        placed = jnp.cumsum(step_flags) - step_flags
        return jnp.minimum(placed, N_DEV - 1).astype(jnp.int32)
    return jax.vmap(one_device)(jax.random.split(jax.random.fold_in(key, 5), groups)).reshape(EDGES)


def draw_coarse_receivers(key, part):
    groups = CEDGES // CE_DEV
    slot_total = groups * CCAP
    full_owner = jax.random.randint(jax.random.fold_in(key, 11), (), 0, groups, dtype=jnp.int32)
    slot_ids = jnp.arange(slot_total, dtype=jnp.int32)
    owner_of = slot_ids // CCAP

    def one_device(dev_key):
        sub_keys = jax.random.split(dev_key, 3)
        scores = jax.random.randint(sub_keys[0], (slot_total,), 0, 1 << 16, dtype=jnp.int32) * slot_total + slot_ids
        scores = jnp.where(owner_of == full_owner, -1 - slot_ids, scores)
        slot_order = jnp.argsort(scores, stable=True)
        chosen = slot_order[:CE_DEV].astype(jnp.int32)
        shuffle_scores = jax.random.randint(sub_keys[1], (CE_DEV,), 0, 1 << 16, dtype=jnp.int32) * CE_DEV + jnp.arange(CE_DEV, dtype=jnp.int32)
        chosen = chosen[jnp.argsort(shuffle_scores, stable=True)]
        node_pick = jax.random.randint(sub_keys[2], (CE_DEV,), 0, NCD, dtype=jnp.int32)
        return (chosen // CCAP * NCD + node_pick).astype(jnp.int32)
    return jax.vmap(one_device)(jax.random.split(jax.random.fold_in(key, 7), groups)).reshape(CEDGES)


def touch_ends(array, rng, smallest, largest):
    shape = array.shape
    index_at = [jax.random.randint(jax.random.fold_in(rng, axis), (), 0, shape[axis]) for axis in range(len(shape))]
    array = array.at[tuple(index_at)].set(smallest)
    longest = shape.index(max(shape))
    index_at[longest] = (index_at[longest] + 1) % shape[longest]
    return array.at[tuple(index_at)].set(largest)


def steps_of(stream_key, extent, cuts, least, top_value):
    gain = 1.0
    for axis_at, parts in cuts:
        heights = jax.random.uniform(jax.random.fold_in(jax.random.fold_in(stream_key, 6), axis_at), (parts,), jnp.float32, least / len(cuts), top_value / len(cuts))
        gain = gain * jnp.repeat(jnp.exp(heights), extent[axis_at] // parts).reshape((-1,) + (1,) * (len(extent) - 1 - axis_at))
    return gain


def noise(stream_key, shape, deviation, reach, cuts=(), kind=jnp.bfloat16):
    entries = jax.random.normal(stream_key, shape, jnp.float32) * deviation
    if len(cuts) > 0:
        entries = steps_of(stream_key, shape, cuts, -0.22, 0.18) * entries
    return jnp.clip(entries, min=-reach, max=reach).astype(kind)


def setup_inputs(seed: int = 0) -> dict:
    arg_keys = jax.random.split(jax.random.key(seed), 21)
    return {
        "node_feats": noise(arg_keys[0], (NODES, D), 1.0, 6.0, ((0, 32),)),
        "edge_feats": noise(arg_keys[1], (EDGES, D), 1.0, 6.0, ((0, 32),)),
        "senders": touch_ends(jax.random.randint(arg_keys[2], (EDGES,), 0, N_DEV + 4 * HB), jax.random.fold_in(arg_keys[2], 1), 0, (N_DEV + 4 * HB) - 1).astype(jnp.int32),
        "receivers": draw_receivers(jax.random.fold_in(arg_keys[20], 71), 0),
        "send_lists": touch_ends(jax.random.randint(arg_keys[4], (HB * N_GX * N_GY,), 0, N_DEV), jax.random.fold_in(arg_keys[4], 1), 0, N_DEV - 1).astype(jnp.int32),
        "coarse_edges": noise(arg_keys[5], (CEDGES, D), 1.0, 6.0, ((0, 32),)),
        "coarse_senders": touch_ends(jax.random.randint(arg_keys[6], (CEDGES,), 0, NC), jax.random.fold_in(arg_keys[6], 1), 0, NC - 1).astype(jnp.int32),
        "coarse_receivers": draw_coarse_receivers(jax.random.fold_in(arg_keys[20], 71), 0),
        "edge_w1": noise(arg_keys[8], (3 * D, D), (3 * D) ** -0.5, 0.15625),
        "edge_b1": noise(arg_keys[9], (D,), 1.0, 4.0, (), jnp.float32),
        "edge_w2": noise(arg_keys[10], (D, D), D ** -0.5, 0.25),
        "edge_b2": noise(arg_keys[11], (D,), 0.5, 3.0, (), jnp.float32),
        "edge_gain": jnp.clip(1.0 + 0.1 * jax.random.normal(arg_keys[12], (D,), jnp.float32), 0.5, 1.5),
        "edge_shift": noise(arg_keys[13], (D,), 0.5, 3.0, (), jnp.float32),
        "node_w1": noise(arg_keys[14], (2 * D, D), (2 * D) ** -0.5, 0.1875),
        "node_b1": noise(arg_keys[15], (D,), 1.0, 4.0, (), jnp.float32),
        "node_w2": noise(arg_keys[16], (D, D), D ** -0.5, 0.25),
        "node_b2": noise(arg_keys[17], (D,), 0.5, 3.0, (), jnp.float32),
        "node_gain": jnp.clip(1.0 + 0.1 * jax.random.normal(arg_keys[18], (D,), jnp.float32), 0.5, 1.5),
        "node_shift": noise(arg_keys[19], (D,), 0.5, 3.0, (), jnp.float32),
    }


def layer_norm(values, gain_vec, shift_vec):
    row_mean = lax.optimization_barrier(jnp.mean(values, -1, keepdims=True))
    centred = values - row_mean
    variance = lax.optimization_barrier(jnp.mean(centred * centred, -1, keepdims=True))
    return centred * lax.rsqrt(variance + 1e-05) * gain_vec + shift_vec

def edge_update(inputs, edge_rows, w_first, b_first, w_second, b_second, gain_vec, shift_vec):
    pre_act = jnp.dot(inputs, w_first, preferred_element_type=jnp.float32) + b_first
    hidden = jax.nn.silu(pre_act).astype(jnp.bfloat16)
    output = jnp.dot(hidden, w_second, preferred_element_type=jnp.float32) + b_second
    message = layer_norm(output, gain_vec, shift_vec)
    return ((edge_rows.astype(jnp.float32) + message).astype(jnp.bfloat16), message.astype(jnp.bfloat16))

def pick_rows(node_block, index_list):
    return node_block[index_list]

def reference(node_feats, edge_feats, senders, receivers, send_lists, coarse_edges, coarse_senders, coarse_receivers, edge_w1, edge_b1, edge_w2, edge_b2, edge_gain, edge_shift, node_w1, node_b1, node_w2, node_b2, node_gain, node_shift):
    groups = N_GX * N_GY
    nodes3 = node_feats.reshape(groups, N_DEV, D)
    lists = send_lists.reshape(groups, HB)
    boundary = jax.vmap(pick_rows)(nodes3, lists).reshape(N_GX, N_GY, HB, D)
    pieces = [jnp.roll(boundary, 1, 0), jnp.roll(boundary, -1, 0), jnp.roll(boundary, 1, 1), jnp.roll(boundary, -1, 1)]
    node_table = jnp.concatenate([nodes3] + [piece.reshape(groups, HB, D) for piece in pieces], 1)

    def per_device(packed):
        table_rows, edge_rows, send_ids, recv_ids = packed
        inputs = jnp.concatenate([edge_rows, table_rows[send_ids], table_rows[recv_ids]], 1)
        updated, message = edge_update(inputs, edge_rows, edge_w1, edge_b1, edge_w2, edge_b2, edge_gain, edge_shift)
        summed = jax.ops.segment_sum(message.astype(jnp.float32), recv_ids, num_segments=N_DEV)
        return (updated, summed)
    new_edges, fine_sum = lax.map(per_device, (node_table, edge_feats.reshape(groups, E_DEV, D), senders.reshape(groups, E_DEV), receivers.reshape(groups, E_DEV)))
    coarse_nodes = nodes3[:, :NCD].reshape(NC, D)
    coarse_in = jnp.concatenate([coarse_edges, coarse_nodes[coarse_senders], coarse_nodes[coarse_receivers]], 1)
    new_coarse, coarse_msg = edge_update(coarse_in, coarse_edges, edge_w1, edge_b1, edge_w2, edge_b2, edge_gain, edge_shift)
    coarse_sum = jax.ops.segment_sum(coarse_msg.astype(jnp.float32), coarse_receivers, num_segments=NC).reshape(groups, NCD, D)
    fine_sum = fine_sum.at[:, :NCD].add(coarse_sum)

    def per_node(packed):
        node_rows, summed = packed
        inputs = jnp.concatenate([node_rows, summed.astype(jnp.bfloat16)], 1)
        pre_act = jnp.dot(inputs, node_w1, preferred_element_type=jnp.float32) + node_b1
        hidden = jax.nn.silu(pre_act).astype(jnp.bfloat16)
        output = jnp.dot(hidden, node_w2, preferred_element_type=jnp.float32) + node_b2
        return (node_rows.astype(jnp.float32) + layer_norm(output, node_gain, node_shift)).astype(jnp.bfloat16)
    new_nodes = lax.map(per_node, (nodes3, fine_sum)).reshape(NODES, D)
    return (new_nodes, new_edges.reshape(EDGES, D), new_coarse)
```

```python
import functools

import jax
import jax.numpy as jnp
from jax import lax
from jax.experimental import pallas as pl
from jax.experimental.pallas import tpu as pltpu
from jax.sharding import PartitionSpec as P

NCD = 20
BLK = 256
WIN = BLK + 16
HEAD = 32
LANES = 128
F32 = jnp.float32
BF16 = jnp.bfloat16


def dotf(lhs, rhs):
    return jnp.dot(lhs, rhs, preferred_element_type=F32)


def silu_half(half):
    return half + half * jnp.tanh(half)


def norm_rows(values, gain, shift):
    centred = values - jnp.mean(values, -1, keepdims=True)
    variance = jnp.mean(centred * centred, -1, keepdims=True)
    return centred * lax.rsqrt(variance + 1e-05) * gain + shift


def put_rows(table, row, values):
    parts = values.shape[1] // LANES
    for part in range(parts):
        table[pl.ds(row * parts + part, values.shape[0], stride=parts), :] = values[
            :, part * LANES : (part + 1) * LANES
        ]


def node_rows(nodes, aggregate, w1, b1, w2, b2, gain, shift):
    width = nodes.shape[1]
    pre = dotf(nodes, w1[:width, :]) + dotf(aggregate, w1[width:, :]) + b1[...]
    hidden = silu_half(0.5 * pre).astype(BF16)
    return (nodes.astype(F32) + norm_rows(dotf(hidden, w2[...]) + b2[...], gain[...], shift[...])).astype(BF16)


def fine_kernel(
    send4, recv4, nodes, halo, edges, recv_lanes, w1, b1, w2, b2, gain, shift,
    nw1, nb1, nw2, nb2, ngain, nshift,
    new_edges, new_nodes, head, send_table, recv_table, picked_a, picked_b, summed,
):
    step = pl.program_id(0)
    last = pl.num_programs(0) - 1
    count, width = nodes.shape
    parts = width // LANES
    rows = BLK

    def pick(block, out):
        base = block * rows
        for row in range(rows):
            first = pl.multiple_of(send4[base + row], parts)
            second = pl.multiple_of(recv4[base + row], parts)
            out[row * parts : (row + 1) * parts, :] = (
                send_table[pl.ds(first, parts), :] + recv_table[pl.ds(second, parts), :]
            )

    @pl.when(step == 0)
    def _():
        summed[...] = jnp.zeros_like(summed)
        for start in range(0, count, rows):
            some = nodes[start : start + rows, :]
            put_rows(send_table, start, dotf(some, w1[width : 2 * width, :]))
            put_rows(recv_table, start, dotf(some, w1[2 * width :, :]) + b1[...])
        for start in range(0, halo.shape[0], rows):
            put_rows(send_table, count + start, dotf(halo[start : start + rows, :], w1[width : 2 * width, :]))
        pick(0, picked_a)

    def update(half, picked):
        edge_rows = edges[half * rows : (half + 1) * rows, :]
        pre = dotf(edge_rows, w1[:width, :])
        hidden = []
        for part in range(parts):
            piece = pre[:, part * LANES : (part + 1) * LANES] + picked[pl.ds(part, rows, stride=parts), :]
            hidden.append(silu_half(0.5 * piece).astype(BF16))
        hidden = jnp.concatenate(hidden, 1)
        message = norm_rows(dotf(hidden, w2[...]) + b2[...], gain[...], shift[...])
        new_edges[half * rows : (half + 1) * rows, :] = (edge_rows.astype(F32) + message).astype(BF16)
        first = recv4[(2 * step + half) * rows] // parts
        first = pl.multiple_of((first // 8) * 8, 8)
        ids = recv_lanes[0, half : half + 1, :] - first
        onehot = (lax.broadcasted_iota(jnp.int32, (WIN, rows), 0) == ids).astype(BF16)
        summed[pl.ds(first, WIN), :] += dotf(onehot, message.astype(BF16))

    pick(2 * step + 1, picked_b)
    update(0, picked_a)
    pick(jnp.minimum(2 * step + 2, 2 * last), picked_a)
    update(1, picked_b)

    @pl.when(step == last)
    def _():
        head[...] = summed[:HEAD, :]
        for start in range(0, count, rows):
            new_nodes[start : start + rows, :] = node_rows(
                nodes[start : start + rows, :], summed[start : start + rows, :].astype(BF16),
                nw1, nb1, nw2, nb2, ngain, nshift,
            )


def whole(shape):
    return pl.BlockSpec(shape, lambda *_: (0,) * len(shape))


def fine_update(nodes, halo, edges, senders, receivers, weights, node_weights):
    count, width = nodes.shape
    edge_count = edges.shape[0]
    parts = width // LANES
    steps = edge_count // (2 * BLK)
    table = count + halo.shape[0]
    operands = (nodes, halo)
    extra = (*weights, *node_weights)
    return pl.pallas_call(
        fine_kernel,
        grid_spec=pltpu.PrefetchScalarGridSpec(
            num_scalar_prefetch=2,
            grid=(steps,),
            in_specs=[whole(item.shape) for item in operands]
            + [
                pl.BlockSpec((2 * BLK, width), lambda i, *_: (i, 0)),
                pl.BlockSpec((1, 2, BLK), lambda i, *_: (i, 0, 0)),
            ]
            + [whole(item.shape) for item in extra],
            out_specs=[
                pl.BlockSpec((2 * BLK, width), lambda i, *_: (i, 0)),
                whole((count, width)),
                whole((HEAD, width)),
            ],
            scratch_shapes=[
                pltpu.VMEM((table * parts, LANES), F32),
                pltpu.VMEM((count * parts, LANES), F32),
                pltpu.VMEM((BLK * parts, LANES), F32),
                pltpu.VMEM((BLK * parts, LANES), F32),
                pltpu.VMEM((count + WIN, width), F32),
            ],
        ),
        out_shape=[
            jax.ShapeDtypeStruct((edge_count, width), BF16),
            jax.ShapeDtypeStruct((count, width), BF16),
            jax.ShapeDtypeStruct((HEAD, width), F32),
        ],
        compiler_params=pltpu.CompilerParams(
            dimension_semantics=("arbitrary",), vmem_limit_bytes=48 << 20
        ),
        name="fine",
    )(
        senders * parts, receivers * parts, *operands, edges,
        receivers.reshape(steps, 2, BLK), *extra,
    )


def tail_kernel(nodes, head, coarse, nw1, nb1, nw2, nb2, ngain, nshift, _, new_nodes):
    aggregate = (head[...] + coarse[...]).astype(BF16)
    new_nodes[...] = node_rows(nodes[...], aggregate, nw1, nb1, nw2, nb2, ngain, nshift)


def tail_update(nodes, head, coarse, node_weights, new_nodes):
    width = nodes.shape[1]
    args = (nodes, head, coarse, *node_weights, new_nodes)
    return pl.pallas_call(
        tail_kernel,
        grid=(1,),
        in_specs=[whole((HEAD, width))] * 3
        + [whole(item.shape) for item in node_weights]
        + [pl.BlockSpec(memory_space=pl.ANY)],
        out_specs=whole((HEAD, width)),
        out_shape=jax.ShapeDtypeStruct(new_nodes.shape, BF16),
        input_output_aliases={len(args) - 1: 0},
        name="tail",
    )(*args)


def layer_norm(values, gain_vec, shift_vec):
    row_mean = jnp.mean(values, -1, keepdims=True)
    centred = values - row_mean
    variance = jnp.mean(centred * centred, -1, keepdims=True)
    return centred * lax.rsqrt(variance + 1e-05) * gain_vec + shift_vec


def finish_edge(pre_act, edge_rows, w_second, b_second, gain_vec, shift_vec):
    hidden = jax.nn.silu(pre_act).astype(BF16)
    output = jnp.dot(hidden, w_second, preferred_element_type=F32) + b_second
    message = layer_norm(output, gain_vec, shift_vec)
    return (edge_rows.astype(F32) + message).astype(BF16), message.astype(BF16)


def shift_ring(count, step):
    return [(item, (item + step) % count) for item in range(count)]


def on_device(
    node_feats, edge_feats, senders, receivers, send_lists, coarse_edges, coarse_senders, coarse_receivers,
    edge_w1, edge_b1, edge_w2, edge_b2, edge_gain, edge_shift,
    node_w1, node_b1, node_w2, node_b2, node_gain, node_shift,
):
    boundary = node_feats[send_lists]
    halo = jnp.concatenate(
        [
            lax.ppermute(boundary, axis, shift_ring(lax.axis_size(axis), step))
            for axis in ("gx", "gy")
            for step in (1, -1)
        ],
        0,
    )
    row = lambda vec: vec[None, :]
    weights = (edge_w1, row(edge_b1), edge_w2, row(edge_b2), row(edge_gain), row(edge_shift))
    node_weights = (node_w1, row(node_b1), node_w2, row(node_b2), row(node_gain), row(node_shift))
    new_edges, new_nodes, head = fine_update(
        node_feats, halo, edge_feats, senders, receivers, weights, node_weights
    )
    coarse_nodes = lax.all_gather(node_feats[:NCD], ("gx", "gy"), axis=0, tiled=True)
    coarse_in = jnp.concatenate(
        [coarse_edges, coarse_nodes[coarse_senders], coarse_nodes[coarse_receivers]], 1
    )
    coarse_pre = jnp.dot(coarse_in, edge_w1, preferred_element_type=F32) + edge_b1
    new_coarse, coarse_msg = finish_edge(
        coarse_pre, coarse_edges, edge_w2, edge_b2, edge_gain, edge_shift
    )
    coarse_count = coarse_nodes.shape[0]
    coarse_hot = (
        coarse_receivers[None, :] == jnp.arange(coarse_count, dtype=jnp.int32)[:, None]
    ).astype(BF16)
    summed_all = lax.psum(jnp.dot(coarse_hot, coarse_msg, preferred_element_type=F32), ("gx", "gy"))
    owned_sum = lax.dynamic_slice_in_dim(summed_all, lax.axis_index(("gx", "gy")) * NCD, NCD, 0)
    owned_sum = jnp.pad(owned_sum, ((0, HEAD - NCD), (0, 0)))
    new_nodes = tail_update(node_feats, head, owned_sum, node_weights, new_nodes)
    return new_nodes, new_edges, new_coarse


def solution(mesh):
    split = P(("gx", "gy"), None)
    flat = P(("gx", "gy"))
    placed = (split, split, flat, flat, flat, split, flat, flat) + (P(),) * 12
    return jax.shard_map(
        on_device, mesh=mesh, in_specs=placed, out_specs=(split, split, split), check_vma=False
    )
```

```python
import functools

import jax
import jax.numpy as jnp
from jax import lax
from jax.experimental import pallas as pl
from jax.experimental.pallas import tpu as pltpu
from jax.sharding import PartitionSpec as P

NCD = 20
BLK = 256
WIN = BLK + 16
HEAD = 32
LOW = 16
VMEM_LIMIT = 60 << 20
LANES = 128
F32 = jnp.float32
BF16 = jnp.bfloat16


def dotf(lhs, rhs):
    return jnp.dot(lhs, rhs, preferred_element_type=F32)


def silu_half(half):
    return half + half * jnp.tanh(half)


def norm_rows(values, gain, shift):
    centred = values - jnp.mean(values, -1, keepdims=True)
    variance = jnp.mean(centred * centred, -1, keepdims=True)
    return centred * lax.rsqrt(variance + 1e-05) * gain + shift


def put_rows(table, row, values):
    parts = values.shape[1] // LANES
    for part in range(parts):
        table[pl.ds(row * parts + part, values.shape[0], stride=parts), :] = values[
            :, part * LANES : (part + 1) * LANES
        ]


def node_rows(nodes, aggregate, w1, b1, w2, b2, gain, shift):
    width = nodes.shape[1]
    pre = dotf(nodes, w1[:width, :]) + dotf(aggregate, w1[width:, :]) + b1[...]
    hidden = silu_half(0.5 * pre).astype(BF16)
    return (nodes.astype(F32) + norm_rows(dotf(hidden, w2[...]) + b2[...], gain[...], shift[...])).astype(BF16)


def fine_kernel(
    send4, recv4, nodes, halo0, halo1, halo2, halo3, edges, recv_lanes, w1, b1, w2, b2, gain, shift,
    nw1, nb1, nw2, nb2, ngain, nshift,
    new_edges, new_nodes, head, send_table, recv_table, picked_a, picked_b, summed,
):
    step = pl.program_id(0)
    last = pl.num_programs(0) - 1
    count, width = nodes.shape
    parts = width // LANES
    rows = BLK

    def pick(block, out):
        base = block * rows
        for row in range(rows):
            first = pl.multiple_of(send4[base + row], parts)
            second = pl.multiple_of(recv4[base + row], parts)
            out[row * parts : (row + 1) * parts, :] = (
                send_table[pl.ds(first, parts), :] + recv_table[pl.ds(second, parts), :]
            )

    @pl.when(step == 0)
    def _():
        summed[...] = jnp.zeros_like(summed)
        for start in range(0, count, rows):
            some = nodes[start : start + rows, :]
            put_rows(send_table, start, dotf(some, w1[width : 2 * width, :]))
            put_rows(recv_table, start, dotf(some, w1[2 * width :, :]) + b1[...])
        start = count
        for halo in (halo0, halo1, halo2, halo3):
            put_rows(send_table, start, dotf(halo[...], w1[width : 2 * width, :]))
            start += halo.shape[0]
        pick(0, picked_a)

    def update(half, picked):
        edge_rows = edges[half * rows : (half + 1) * rows, :]
        pre = dotf(edge_rows, w1[:width, :])
        hidden = []
        for part in range(parts):
            piece = pre[:, part * LANES : (part + 1) * LANES] + picked[pl.ds(part, rows, stride=parts), :]
            hidden.append(silu_half(0.5 * piece).astype(BF16))
        hidden = jnp.concatenate(hidden, 1)
        message = norm_rows(dotf(hidden, w2[...]) + b2[...], gain[...], shift[...])
        new_edges[half * rows : (half + 1) * rows, :] = (edge_rows.astype(F32) + message).astype(BF16)
        first = recv4[(2 * step + half) * rows] // parts
        first = pl.multiple_of((first // 8) * 8, 8)
        ids = recv_lanes[0, half : half + 1, :] - first
        onehot = (lax.broadcasted_iota(jnp.int32, (WIN, rows), 0) == ids).astype(BF16)
        summed[pl.ds(first, WIN), :] += dotf(onehot, message.astype(BF16))

    pick(2 * step + 1, picked_b)
    update(0, picked_a)
    pick(jnp.minimum(2 * step + 2, 2 * last), picked_a)
    update(1, picked_b)

    @pl.when(step == last)
    def _():
        head[...] = summed[:HEAD, :]
        for start in range(0, count, rows):
            new_nodes[start : start + rows, :] = node_rows(
                nodes[start : start + rows, :], summed[start : start + rows, :].astype(BF16),
                nw1, nb1, nw2, nb2, ngain, nshift,
            )


def whole(shape):
    return pl.BlockSpec(shape, lambda *_: (0,) * len(shape))


def fine_update(nodes, halos, edges, senders, receivers, weights, node_weights):
    count, width = nodes.shape
    edge_count = edges.shape[0]
    parts = width // LANES
    steps = edge_count // (2 * BLK)
    table = count + sum(halo.shape[0] for halo in halos)
    operands = (nodes, *halos)
    extra = (*weights, *node_weights)
    return pl.pallas_call(
        fine_kernel,
        grid_spec=pltpu.PrefetchScalarGridSpec(
            num_scalar_prefetch=2,
            grid=(steps,),
            in_specs=[whole(item.shape) for item in operands]
            + [
                pl.BlockSpec((2 * BLK, width), lambda i, *_: (i, 0)),
                pl.BlockSpec((1, 2, BLK), lambda i, *_: (i, 0, 0)),
            ]
            + [whole(item.shape) for item in extra],
            out_specs=[
                pl.BlockSpec((2 * BLK, width), lambda i, *_: (i, 0)),
                whole((count, width)),
                whole((HEAD, width)),
            ],
            scratch_shapes=[
                pltpu.VMEM((table * parts, LANES), F32),
                pltpu.VMEM((count * parts, LANES), F32),
                pltpu.VMEM((BLK * parts, LANES), F32),
                pltpu.VMEM((BLK * parts, LANES), F32),
                pltpu.VMEM((count + WIN, width), F32),
            ],
        ),
        out_shape=[
            jax.ShapeDtypeStruct((edge_count, width), BF16),
            jax.ShapeDtypeStruct((count, width), BF16),
            jax.ShapeDtypeStruct((HEAD, width), F32),
        ],
        cost_estimate=pl.CostEstimate(
            flops=edge_count * width * width * 6, transcendentals=0, bytes_accessed=16 << 20
        ),
        compiler_params=pltpu.CompilerParams(
            dimension_semantics=("arbitrary",), vmem_limit_bytes=VMEM_LIMIT
        ),
        name="fine",
    )(
        senders * parts, receivers * parts, *operands, edges,
        receivers.reshape(steps, 2, BLK), *extra,
    )


def row_floor(values, divisor):
    return jnp.floor((values + 0.5) * (1.0 / divisor))


def pair_rows(cap):
    return -(-(NCD + cap + 1) // LOW) * LOW


def iota(shape, dim):
    return lax.broadcasted_iota(jnp.int32, shape, dim)


def contract(lhs, rhs, dims):
    return lax.dot_general(lhs, rhs, ((dims[:1], dims[1:]), ((), ())), preferred_element_type=F32)


def prologue_kernel(devices, cap, nodes, send_list, edges, senders, receivers, boundary, parcel, own):
    count, width = edges.shape
    rows = parcel.shape[0] // devices
    high = rows - LOW

    def split(ids):
        owner = row_floor(ids, NCD)
        return owner, ids - owner * NCD

    send_owner, send_local = split(senders[...].astype(F32))
    recv_owner, recv_local = split(receivers[...].astype(F32))
    row_at = iota((count, count), 0)
    col_at = iota((count, count), 1)
    eye = (row_at == col_at).astype(BF16)
    line = iota((LANES, count), 0)

    def columns(items):
        out = jnp.zeros((LANES, count), F32)
        for at, item in enumerate(items):
            out = jnp.where(line == at, item, out)
        return contract(eye, out.astype(BF16), (1, 1))

    cols = columns([send_owner, send_local, recv_owner, recv_local])
    own[...] = cols.astype(BF16)
    owner_col = cols[:, 2:3]
    before = jnp.where((owner_col == recv_owner) & (row_at < col_at), 1.0, 0.0)
    rank = jnp.sum(before, 0, keepdims=True)
    rank_col = columns([rank])[:, :1]
    where_to = recv_owner * high + (NCD - LOW)
    slot = (where_to + rank).astype(jnp.int32)
    place = (where_to + cap).astype(jnp.int32)
    total = devices * high
    at_row = iota((total, count), 0)
    lane = iota((count, LANES), 1).astype(F32)
    here = lane == rank_col
    index_rows = [jnp.where(here, item, 0.0) for item in (cols[:, 0:1], cols[:, 1:2], cols[:, 3:4] + 1.0)]
    index_rows.append(jnp.zeros((count, width - 3 * LANES), F32))
    index_rows = jnp.concatenate(index_rows, 1).astype(BF16)
    sent = dotf((at_row == slot).astype(BF16), edges[...]) + dotf((at_row == place).astype(BF16), index_rows)
    first = nodes[:LOW, :]
    second = nodes[LOW : LOW + high, :].astype(F32)
    second = jnp.where(iota((high, width), 0) < NCD - LOW, second, 0.0)
    for device in range(devices):
        parcel[device * rows : device * rows + LOW, :] = first
        parcel[device * rows + LOW : (device + 1) * rows, :] = (
            sent[device * high : (device + 1) * high, :] + second
        ).astype(BF16)
    pick = (iota((nodes.shape[0], send_list.shape[1]), 0) == send_list[...]).astype(BF16)
    boundary[...] = contract(pick, nodes[...], (0, 0)).astype(BF16)


def prologue(devices, cap, nodes, send_list, edges, senders, receivers):
    width = nodes.shape[1]
    args = (nodes, send_list[None, :], edges, senders[None, :], receivers[None, :])
    shapes = [
        (send_list.shape[0], width), (devices * pair_rows(cap), width), (edges.shape[0], LANES)
    ]
    return pl.pallas_call(
        functools.partial(prologue_kernel, devices, cap),
        grid=(1,),
        in_specs=[whole(item.shape) for item in args],
        out_specs=[whole(shape) for shape in shapes],
        out_shape=[jax.ShapeDtypeStruct(shape, BF16) for shape in shapes],
        compiler_params=pltpu.CompilerParams(vmem_limit_bytes=VMEM_LIMIT),
        name="prologue",
    )(*args)


def coarse_kernel(
    devices, cap, parcel, edges, own, nodes, head, w1, b1, w2, b2, gain, shift,
    nw1, nb1, nw2, nb2, ngain, nshift, _, new_edges, new_nodes,
):
    width = edges.shape[1]
    total = parcel.shape[0]
    rows = total // devices
    high = rows - LOW

    def messages(edge_rows, send_rows, recv_rows):
        pre = dotf(edge_rows, w1[:width, :]) + dotf(send_rows, w1[width : 2 * width, :])
        pre = pre + dotf(recv_rows, w1[2 * width :, :]) + b1[...]
        hidden = silu_half(0.5 * pre).astype(BF16)
        return norm_rows(dotf(hidden, w2[...]) + b2[...], gain[...], shift[...])

    def lookup(owner, local):
        at = (owner * rows + local).astype(jnp.int32)
        hot = (iota((owner.shape[0], total), 1) == at).astype(BF16)
        return dotf(hot, parcel[...]).astype(BF16)

    tops = jnp.concatenate(
        [parcel[device * rows + LOW : (device + 1) * rows, :] for device in range(devices)], 0
    )
    slots = devices * cap
    column = iota((slots, 1), 0).astype(F32)
    source = row_floor(column, cap)
    rank = column - source * cap
    column_at = iota((slots, devices * high), 1)

    def top_rows(offset):
        at = (source * high + offset).astype(jnp.int32)
        return dotf((column_at == at).astype(BF16), tops)

    edge_rows = top_rows(rank + (NCD - LOW)).astype(BF16)
    index_rows = top_rows(float(NCD - LOW + cap))
    here = iota((slots, LANES), 1).astype(F32) == rank

    def index(part):
        some = index_rows[:, part * LANES : (part + 1) * LANES]
        return jnp.sum(jnp.where(here, some, 0.0), 1, keepdims=True)

    send_rows = lookup(index(0), index(1))
    hot = (iota((slots, LANES), 1) == index(2).astype(jnp.int32) - 1).astype(BF16)
    recv_rows = dotf(hot, nodes[...]).astype(BF16)
    message = messages(edge_rows, send_rows, recv_rows).astype(BF16)
    coarse = contract(hot, message, (0, 0))
    aggregate = (head[...] + coarse[:HEAD, :]).astype(BF16)
    new_nodes[...] = node_rows(nodes[:HEAD, :], aggregate, nw1, nb1, nw2, nb2, ngain, nshift)
    meta = own[...].astype(F32)
    message = messages(edges[...], lookup(meta[:, 0:1], meta[:, 1:2]), lookup(meta[:, 2:3], meta[:, 3:4]))
    new_edges[...] = (edges[...].astype(F32) + message).astype(BF16)


def coarse_update(devices, cap, parcel, edges, own, nodes, head, weights, node_weights, new_nodes):
    width = nodes.shape[1]
    args = (parcel, edges, own, nodes, head, *weights, *node_weights, new_nodes)
    specs = [whole(item.shape) for item in args]
    specs[3] = whole((LANES, width))
    specs[-1] = pl.BlockSpec(memory_space=pl.ANY)
    return pl.pallas_call(
        functools.partial(coarse_kernel, devices, cap),
        grid=(1,),
        in_specs=specs,
        out_specs=[whole(edges.shape), whole((HEAD, width))],
        out_shape=[
            jax.ShapeDtypeStruct(edges.shape, BF16),
            jax.ShapeDtypeStruct(new_nodes.shape, BF16),
        ],
        input_output_aliases={len(args) - 1: 1},
        compiler_params=pltpu.CompilerParams(vmem_limit_bytes=VMEM_LIMIT),
        name="coarse",
    )(*args)


def shift_ring(count, step):
    return [(item, (item + step) % count) for item in range(count)]


def on_device(
    node_feats, edge_feats, senders, receivers, send_lists, coarse_edges, coarse_senders, coarse_receivers,
    edge_w1, edge_b1, edge_w2, edge_b2, edge_gain, edge_shift,
    node_w1, node_b1, node_w2, node_b2, node_gain, node_shift,
):
    axes = ("gx", "gy")
    devices = lax.axis_size(axes)
    cap = -(-2 * coarse_edges.shape[0] // devices)
    row = lambda vec: vec[None, :]
    weights = (edge_w1, row(edge_b1), edge_w2, row(edge_b2), row(edge_gain), row(edge_shift))
    node_weights = (node_w1, row(node_b1), node_w2, row(node_b2), row(node_gain), row(node_shift))
    boundary, parcel, own = prologue(
        devices, cap, node_feats, send_lists, coarse_edges, coarse_senders, coarse_receivers
    )
    parcel = lax.all_to_all(parcel, axes, 0, 0, tiled=True)
    halos = [
        lax.ppermute(boundary, axis, shift_ring(lax.axis_size(axis), step))
        for axis in axes
        for step in (1, -1)
    ]
    new_edges, new_nodes, head = fine_update(
        node_feats, halos, edge_feats, senders, receivers, weights, node_weights
    )
    new_coarse, new_nodes = coarse_update(
        devices, cap, parcel, coarse_edges, own, node_feats, head, weights, node_weights, new_nodes
    )
    return new_nodes, new_edges, new_coarse


def solution(mesh):
    split = P(("gx", "gy"), None)
    flat = P(("gx", "gy"))
    placed = (split, split, flat, flat, flat, split, flat, flat) + (P(),) * 12
    return jax.shard_map(
        on_device, mesh=mesh, in_specs=placed, out_specs=(split, split, split), check_vma=False
    )
```

```python
import functools

import jax
import jax.numpy as jnp
from jax import lax
from jax.experimental import pallas as pl
from jax.experimental.pallas import tpu as pltpu
from jax.sharding import PartitionSpec as P


NCD = 20
BLK = 256
WIN = BLK + 16
HEAD = 32
LOW = 16
VMEM_LIMIT = 60 << 20
LANES = 128
F32 = jnp.float32
BF16 = jnp.bfloat16


def dotf(lhs, rhs):
    return jnp.dot(lhs, rhs, preferred_element_type=F32)


def silu_half(half):
    return half + half * jnp.tanh(half)


def norm_rows(values, gain, shift):
    centred = values - jnp.mean(values, -1, keepdims=True)
    variance = jnp.mean(centred * centred, -1, keepdims=True)
    return centred * lax.rsqrt(variance + 1e-05) * gain + shift


def put_rows(table, row, values):
    parts = values.shape[1] // LANES
    for part in range(parts):
        table[pl.ds(row * parts + part, values.shape[0], stride=parts), :] = values[
            :, part * LANES : (part + 1) * LANES
        ]


def node_rows(nodes, aggregate, w1, b1, w2, b2, gain, shift):
    width = nodes.shape[1]
    pre = dotf(nodes, w1[:width, :]) + dotf(aggregate, w1[width:, :]) + b1[...]
    hidden = silu_half(0.5 * pre).astype(BF16)
    return (nodes.astype(F32) + norm_rows(dotf(hidden, w2[...]) + b2[...], gain[...], shift[...])).astype(BF16)


def fine_kernel(
    send4, recv4, nodes, halo0, halo1, halo2, halo3, edges, recv_lanes, w1, b1, w2, b2, gain, shift,
    nw1, nb1, nw2, nb2, ngain, nshift,
    new_edges, new_nodes, head, send_table, recv_table, picked_a, picked_b, summed,
):
    step = pl.program_id(0)
    last = pl.num_programs(0) - 1
    count, width = nodes.shape
    parts = width // LANES
    rows = BLK

    def pick(block, out):
        base = block * rows
        for row in range(rows):
            first = pl.multiple_of(send4[base + row], parts)
            second = pl.multiple_of(recv4[base + row], parts)
            out[row * parts : (row + 1) * parts, :] = (
                send_table[pl.ds(first, parts), :] + recv_table[pl.ds(second, parts), :]
            )

    @pl.when(step == 0)
    def _():
        summed[...] = jnp.zeros_like(summed)
        for start in range(0, count, rows):
            some = nodes[start : start + rows, :]
            put_rows(send_table, start, dotf(some, w1[width : 2 * width, :]))
            put_rows(recv_table, start, dotf(some, w1[2 * width :, :]) + b1[...])
        start = count
        for halo in (halo0, halo1, halo2, halo3):
            put_rows(send_table, start, dotf(halo[...], w1[width : 2 * width, :]))
            start += halo.shape[0]
        pick(0, picked_a)

    def update(half, picked):
        edge_rows = edges[half * rows : (half + 1) * rows, :]
        pre = dotf(edge_rows, w1[:width, :])
        hidden = []
        for part in range(parts):
            piece = pre[:, part * LANES : (part + 1) * LANES] + picked[pl.ds(part, rows, stride=parts), :]
            hidden.append(silu_half(0.5 * piece).astype(BF16))
        hidden = jnp.concatenate(hidden, 1)
        message = norm_rows(dotf(hidden, w2[...]) + b2[...], gain[...], shift[...])
        new_edges[half * rows : (half + 1) * rows, :] = (edge_rows.astype(F32) + message).astype(BF16)
        first = recv4[(2 * step + half) * rows] // parts
        first = pl.multiple_of((first // 8) * 8, 8)
        ids = recv_lanes[0, half : half + 1, :] - first
        onehot = (lax.broadcasted_iota(jnp.int32, (WIN, rows), 0) == ids).astype(BF16)
        summed[pl.ds(first, WIN), :] += dotf(onehot, message.astype(BF16))

    pick(2 * step + 1, picked_b)
    update(0, picked_a)
    pick(jnp.minimum(2 * step + 2, 2 * last), picked_a)
    update(1, picked_b)

    @pl.when(step == last)
    def _():
        head[...] = summed[:HEAD, :]
        for start in range(0, count, rows):
            new_nodes[start : start + rows, :] = node_rows(
                nodes[start : start + rows, :], summed[start : start + rows, :].astype(BF16),
                nw1, nb1, nw2, nb2, ngain, nshift,
            )


def whole(shape):
    return pl.BlockSpec(shape, lambda *_: (0,) * len(shape))


def fine_update(nodes, halos, edges, senders, receivers, weights, node_weights):
    count, width = nodes.shape
    edge_count = edges.shape[0]
    parts = width // LANES
    steps = edge_count // (2 * BLK)
    table = count + sum(halo.shape[0] for halo in halos)
    operands = (nodes, *halos)
    extra = (*weights, *node_weights)
    return pl.pallas_call(
        fine_kernel,
        grid_spec=pltpu.PrefetchScalarGridSpec(
            num_scalar_prefetch=2,
            grid=(steps,),
            in_specs=[whole(item.shape) for item in operands]
            + [
                pl.BlockSpec((2 * BLK, width), lambda i, *_: (i, 0)),
                pl.BlockSpec((1, 2, BLK), lambda i, *_: (i, 0, 0)),
            ]
            + [whole(item.shape) for item in extra],
            out_specs=[
                pl.BlockSpec((2 * BLK, width), lambda i, *_: (i, 0)),
                whole((count, width)),
                whole((HEAD, width)),
            ],
            scratch_shapes=[
                pltpu.VMEM((table * parts, LANES), F32),
                pltpu.VMEM((count * parts, LANES), F32),
                pltpu.VMEM((BLK * parts, LANES), F32),
                pltpu.VMEM((BLK * parts, LANES), F32),
                pltpu.VMEM((count + WIN, width), F32),
            ],
        ),
        out_shape=[
            jax.ShapeDtypeStruct((edge_count, width), BF16),
            jax.ShapeDtypeStruct((count, width), BF16),
            jax.ShapeDtypeStruct((HEAD, width), F32),
        ],
        cost_estimate=pl.CostEstimate(
            flops=edge_count * width * width * 6, transcendentals=0, bytes_accessed=16 << 20
        ),
        compiler_params=pltpu.CompilerParams(
            dimension_semantics=("arbitrary",), vmem_limit_bytes=VMEM_LIMIT
        ),
        name="fine",
    )(
        senders * parts, receivers * parts, *operands, edges,
        receivers.reshape(steps, 2, BLK), *extra,
    )


def row_floor(values, divisor):
    return jnp.floor((values + 0.5) * (1.0 / divisor))


def pair_rows(cap):
    return -(-(NCD + cap + 1) // LOW) * LOW


def iota(shape, dim):
    return lax.broadcasted_iota(jnp.int32, shape, dim)


def contract(lhs, rhs, dims):
    return lax.dot_general(lhs, rhs, ((dims[:1], dims[1:]), ((), ())), preferred_element_type=F32)


def prologue_kernel(devices, cap, nodes, send_list, edges, senders, receivers, boundary, parcel, own):
    count, width = edges.shape
    rows = parcel.shape[0] // devices
    high = rows - LOW

    def split(ids):
        owner = row_floor(ids, NCD)
        return owner, ids - owner * NCD

    send_owner, send_local = split(senders[...].astype(F32))
    recv_owner, recv_local = split(receivers[...].astype(F32))
    row_at = iota((count, count), 0)
    col_at = iota((count, count), 1)
    eye = (row_at == col_at).astype(BF16)
    line = iota((LANES, count), 0)

    def columns(items):
        out = jnp.zeros((LANES, count), F32)
        for at, item in enumerate(items):
            out = jnp.where(line == at, item, out)
        return contract(eye, out.astype(BF16), (1, 1))

    cols = columns([send_owner, send_local, recv_owner, recv_local])
    own[...] = cols.astype(BF16)
    owner_col = cols[:, 2:3]
    before = jnp.where((owner_col == recv_owner) & (row_at < col_at), 1.0, 0.0)
    rank = jnp.sum(before, 0, keepdims=True)
    rank_col = columns([rank])[:, :1]
    where_to = recv_owner * high + (NCD - LOW)
    slot = (where_to + rank).astype(jnp.int32)
    place = (where_to + cap).astype(jnp.int32)
    total = devices * high
    at_row = iota((total, count), 0)
    lane = iota((count, LANES), 1).astype(F32)
    here = lane == rank_col
    index_rows = [jnp.where(here, item, 0.0) for item in (cols[:, 0:1], cols[:, 1:2], cols[:, 3:4] + 1.0)]
    index_rows.append(jnp.zeros((count, width - 3 * LANES), F32))
    index_rows = jnp.concatenate(index_rows, 1).astype(BF16)
    sent = dotf((at_row == slot).astype(BF16), edges[...]) + dotf((at_row == place).astype(BF16), index_rows)
    first = nodes[:LOW, :]
    second = nodes[LOW : LOW + high, :].astype(F32)
    second = jnp.where(iota((high, width), 0) < NCD - LOW, second, 0.0)
    for device in range(devices):
        parcel[device * rows : device * rows + LOW, :] = first
        parcel[device * rows + LOW : (device + 1) * rows, :] = (
            sent[device * high : (device + 1) * high, :] + second
        ).astype(BF16)
    pick = (iota((nodes.shape[0], send_list.shape[1]), 0) == send_list[...]).astype(BF16)
    boundary[...] = contract(pick, nodes[...], (0, 0)).astype(BF16)


def prologue(devices, cap, nodes, send_list, edges, senders, receivers):
    width = nodes.shape[1]
    args = (nodes, send_list[None, :], edges, senders[None, :], receivers[None, :])
    shapes = [
        (send_list.shape[0], width), (devices * pair_rows(cap), width), (edges.shape[0], LANES)
    ]
    return pl.pallas_call(
        functools.partial(prologue_kernel, devices, cap),
        grid=(1,),
        in_specs=[whole(item.shape) for item in args],
        out_specs=[whole(shape) for shape in shapes],
        out_shape=[jax.ShapeDtypeStruct(shape, BF16) for shape in shapes],
        compiler_params=pltpu.CompilerParams(vmem_limit_bytes=VMEM_LIMIT),
        name="prologue",
    )(*args)


def coarse_kernel(
    devices, cap, parcel, edges, own, nodes, head, w1, b1, w2, b2, gain, shift,
    nw1, nb1, nw2, nb2, ngain, nshift, _, new_edges, new_nodes,
):
    width = edges.shape[1]
    total = parcel.shape[0]
    rows = total // devices
    high = rows - LOW

    def messages(edge_rows, send_rows, recv_rows):
        pre = dotf(edge_rows, w1[:width, :]) + dotf(send_rows, w1[width : 2 * width, :])
        pre = pre + dotf(recv_rows, w1[2 * width :, :]) + b1[...]
        hidden = silu_half(0.5 * pre).astype(BF16)
        return norm_rows(dotf(hidden, w2[...]) + b2[...], gain[...], shift[...])

    def lookup(owner, local):
        at = (owner * rows + local).astype(jnp.int32)
        hot = (iota((owner.shape[0], total), 1) == at).astype(BF16)
        return dotf(hot, parcel[...]).astype(BF16)

    tops = jnp.concatenate(
        [parcel[device * rows + LOW : (device + 1) * rows, :] for device in range(devices)], 0
    )
    slots = devices * cap
    column = iota((slots, 1), 0).astype(F32)
    source = row_floor(column, cap)
    rank = column - source * cap
    column_at = iota((slots, devices * high), 1)

    def top_rows(offset):
        at = (source * high + offset).astype(jnp.int32)
        return dotf((column_at == at).astype(BF16), tops)

    edge_rows = top_rows(rank + (NCD - LOW)).astype(BF16)
    index_rows = top_rows(float(NCD - LOW + cap))
    here = iota((slots, LANES), 1).astype(F32) == rank

    def index(part):
        some = index_rows[:, part * LANES : (part + 1) * LANES]
        return jnp.sum(jnp.where(here, some, 0.0), 1, keepdims=True)

    send_rows = lookup(index(0), index(1))
    hot = (iota((slots, LANES), 1) == index(2).astype(jnp.int32) - 1).astype(BF16)
    recv_rows = dotf(hot, nodes[...]).astype(BF16)
    message = messages(edge_rows, send_rows, recv_rows).astype(BF16)
    coarse = contract(hot, message, (0, 0))
    aggregate = (head[...] + coarse[:HEAD, :]).astype(BF16)
    new_nodes[...] = node_rows(nodes[:HEAD, :], aggregate, nw1, nb1, nw2, nb2, ngain, nshift)
    meta = own[...].astype(F32)
    message = messages(edges[...], lookup(meta[:, 0:1], meta[:, 1:2]), lookup(meta[:, 2:3], meta[:, 3:4]))
    new_edges[...] = (edges[...].astype(F32) + message).astype(BF16)


def coarse_update(devices, cap, parcel, edges, own, nodes, head, weights, node_weights, new_nodes):
    width = nodes.shape[1]
    args = (parcel, edges, own, nodes, head, *weights, *node_weights, new_nodes)
    specs = [whole(item.shape) for item in args]
    specs[3] = whole((LANES, width))
    specs[-1] = pl.BlockSpec(memory_space=pl.ANY)
    return pl.pallas_call(
        functools.partial(coarse_kernel, devices, cap),
        grid=(1,),
        in_specs=specs,
        out_specs=[whole(edges.shape), whole((HEAD, width))],
        out_shape=[
            jax.ShapeDtypeStruct(edges.shape, BF16),
            jax.ShapeDtypeStruct(new_nodes.shape, BF16),
        ],
        input_output_aliases={len(args) - 1: 1},
        compiler_params=pltpu.CompilerParams(vmem_limit_bytes=VMEM_LIMIT),
        name="coarse",
    )(*args)


def shift_ring(count, step):
    return [(item, (item + step) % count) for item in range(count)]


def on_device(
    node_feats, edge_feats, senders, receivers, send_lists, coarse_edges, coarse_senders, coarse_receivers,
    edge_w1, edge_b1, edge_w2, edge_b2, edge_gain, edge_shift,
    node_w1, node_b1, node_w2, node_b2, node_gain, node_shift,
):
    axes = ("gx", "gy")
    devices = lax.axis_size(axes)
    cap = -(-2 * coarse_edges.shape[0] // devices)
    row = lambda vec: vec[None, :]
    weights = (edge_w1, row(edge_b1), edge_w2, row(edge_b2), row(edge_gain), row(edge_shift))
    node_weights = (node_w1, row(node_b1), node_w2, row(node_b2), row(node_gain), row(node_shift))
    boundary, parcel, own = prologue(
        devices, cap, node_feats, send_lists, coarse_edges, coarse_senders, coarse_receivers
    )
    halos = [lax.ppermute(boundary, axis, shift_ring(lax.axis_size(axis), step)) for axis in axes for step in (1, -1)]
    parcel = lax.all_to_all(parcel, axes, 0, 0, tiled=True)
    new_edges, new_nodes, head = fine_update(
        node_feats, halos, edge_feats, senders, receivers, weights, node_weights
    )
    new_coarse, new_nodes = coarse_update(
        devices, cap, parcel, coarse_edges, own, node_feats, head, weights, node_weights, new_nodes
    )
    return new_nodes, new_edges, new_coarse


def solution(mesh):
    split = P(("gx", "gy"), None)
    flat = P(("gx", "gy"))
    placed = (split, split, flat, flat, flat, split, flat, flat) + (P(),) * 12
    return jax.shard_map(
        on_device, mesh=mesh, in_specs=placed, out_specs=(split, split, split), check_vma=False
    )
```

```python
import functools

import jax
import jax.numpy as jnp
from jax import lax
from jax.experimental import pallas as pl
from jax.experimental.pallas import tpu as pltpu
from jax.sharding import PartitionSpec as P


NCD = 20
BLK = 256
WIN = BLK + 16
HEAD = 32
LOW = 16
CHUNK = 64
VMEM_LIMIT = 60 << 20
LANES = 128
F32 = jnp.float32
BF16 = jnp.bfloat16


def dotf(lhs, rhs):
    return jnp.dot(lhs, rhs, preferred_element_type=F32)


def silu_half(half):
    return half + half * jnp.tanh(half)


def norm_rows(values, gain, shift):
    centred = values - jnp.mean(values, -1, keepdims=True)
    variance = jnp.mean(centred * centred, -1, keepdims=True)
    return centred * lax.rsqrt(variance + 1e-05) * gain + shift


def put_rows(table, row, values):
    parts = values.shape[1] // LANES
    for part in range(parts):
        table[pl.ds(row * parts + part, values.shape[0], stride=parts), :] = values[
            :, part * LANES : (part + 1) * LANES
        ]


def node_rows(nodes, aggregate, w1, b1, w2, b2, gain, shift):
    width = nodes.shape[1]
    pre = dotf(nodes, w1[:width, :]) + dotf(aggregate, w1[width:, :]) + b1[...]
    hidden = silu_half(0.5 * pre).astype(BF16)
    return (nodes.astype(F32) + norm_rows(dotf(hidden, w2[...]) + b2[...], gain[...], shift[...])).astype(BF16)


def fine_kernel(
    send_far, recv_far, nodes, halo0, halo1, halo2, halo3, edges, recv_lanes, w1, b1, w2, b2, gain, shift,
    nw1_far, nb1, nw2_far, nb2, ngain, nshift,
    new_edges, new_nodes, head,
    send_table, recv_table, picked_a, picked_b, hidden_a, hidden_b, message_a, message_b, summed, nw1, nw2,
    send4, recv4, sems,
):
    step = pl.program_id(0)
    last = pl.num_programs(0) - 1
    count, width = nodes.shape
    parts = width // LANES
    rows = BLK
    copies = [
        pltpu.make_async_copy(nw1_far, nw1, sems.at[0]),
        pltpu.make_async_copy(nw2_far, nw2, sems.at[1]),
    ]
    index_copies = [
        pltpu.make_async_copy(send_far, send4, sems.at[2]),
        pltpu.make_async_copy(recv_far, recv4, sems.at[3]),
    ]

    def pick(block, out, start, stop):
        base = block * rows
        for row in range(start, stop):
            first = pl.multiple_of(send4[base + row], parts)
            second = pl.multiple_of(recv4[base + row], parts)
            out[row * parts : (row + 1) * parts, :] = (
                send_table[pl.ds(first, parts), :] + recv_table[pl.ds(second, parts), :]
            )

    @pl.when(step == 0)
    def _():
        for copy in index_copies + copies:
            copy.start()
        summed[...] = jnp.zeros_like(summed)
        for start in range(0, count, rows):
            some = nodes[start : start + rows, :]
            put_rows(send_table, start, dotf(some, w1[width : 2 * width, :]))
            put_rows(recv_table, start, dotf(some, w1[2 * width :, :]) + b1[...])
        start = count
        for halo in (halo0, halo1, halo2, halo3):
            put_rows(send_table, start, dotf(halo[...], w1[width : 2 * width, :]))
            start += halo.shape[0]
        for copy in index_copies:
            copy.wait()
        pick(0, picked_a, 0, rows)

    def first_layer(half):
        return dotf(edges[half * rows : (half + 1) * rows, :], w1[:width, :])

    def activate(pre, picked, hidden, start, stop):
        for part in range(parts):
            lanes = slice(part * LANES, (part + 1) * LANES)
            near = picked[pl.ds(start * parts + part, stop - start, stride=parts), :]
            hidden[start:stop, lanes] = silu_half(0.5 * (pre[start:stop, lanes] + near)).astype(BF16)

    def finish(half, out, message, start, stop):
        values = norm_rows(out[start:stop, :] + b2[...], gain[...], shift[...])
        message[start:stop, :] = values.astype(BF16)
        at = slice(half * rows + start, half * rows + stop)
        new_edges[at, :] = (edges[at, :].astype(F32) + values).astype(BF16)

    def collect(half, message):
        first = recv4[(2 * step + half) * rows] // parts
        first = pl.multiple_of((first // 8) * 8, 8)
        ids = recv_lanes[0, half : half + 1, :] - first
        onehot = (lax.broadcasted_iota(jnp.int32, (WIN, rows), 0) == ids).astype(BF16)
        summed[pl.ds(first, WIN), :] += dotf(onehot, message[...])

    chunks = [(start, start + CHUNK) for start in range(0, rows, CHUNK)]
    after = jnp.minimum(2 * step + 2, 2 * last)
    pre_a = first_layer(0)
    for start, stop in chunks:
        activate(pre_a, picked_a, hidden_a, start, stop)
        pick(2 * step + 1, picked_b, start, stop)
    pre_b = first_layer(1)
    out_a = dotf(hidden_a[...], w2[...])
    for start, stop in chunks:
        activate(pre_b, picked_b, hidden_b, start, stop)
        finish(0, out_a, message_a, start, stop)
    out_b = dotf(hidden_b[...], w2[...])
    collect(0, message_a)
    for start, stop in chunks:
        finish(1, out_b, message_b, start, stop)
        pick(after, picked_a, start, stop)
    collect(1, message_b)

    @pl.when(step == last)
    def _():
        for copy in copies:
            copy.wait()
        head[...] = summed[:HEAD, :]
        for start in range(0, count, rows):
            new_nodes[start : start + rows, :] = node_rows(
                nodes[start : start + rows, :], summed[start : start + rows, :].astype(BF16),
                nw1, nb1, nw2, nb2, ngain, nshift,
            )


def whole(shape):
    return pl.BlockSpec(shape, lambda *_: (0,) * len(shape))


def fine_update(nodes, halos, edges, senders, receivers, weights, node_weights):
    count, width = nodes.shape
    edge_count = edges.shape[0]
    parts = width // LANES
    steps = edge_count // (2 * BLK)
    table = count + sum(halo.shape[0] for halo in halos)
    operands = (nodes, *halos)
    extra = (*weights, *node_weights)
    return pl.pallas_call(
        fine_kernel,
        grid_spec=pltpu.PrefetchScalarGridSpec(
            num_scalar_prefetch=0,
            grid=(steps,),
            in_specs=[pl.BlockSpec(memory_space=pl.ANY)] * 2
            + [whole(nodes.shape)] + [pl.BlockSpec(memory_space=pltpu.VMEM)] * len(halos)
            + [
                pl.BlockSpec((2 * BLK, width), lambda i, *_: (i, 0)),
                pl.BlockSpec((1, 2, BLK), lambda i, *_: (i, 0, 0)),
            ]
            + [
                pl.BlockSpec(memory_space=pl.ANY) if at in (6, 8) else whole(item.shape)
                for at, item in enumerate(extra)
            ],
            out_specs=[
                pl.BlockSpec((2 * BLK, width), lambda i, *_: (i, 0)),
                whole((count, width)),
                whole((HEAD, width)),
            ],
            scratch_shapes=[
                pltpu.VMEM((table * parts, LANES), F32),
                pltpu.VMEM((count * parts, LANES), F32),
                pltpu.VMEM((BLK * parts, LANES), F32),
                pltpu.VMEM((BLK * parts, LANES), F32),
            ]
            + [pltpu.VMEM((BLK, width), BF16)] * 4
            + [
                pltpu.VMEM((count + WIN, width), F32),
                pltpu.VMEM(node_weights[0].shape, BF16),
                pltpu.VMEM(node_weights[2].shape, BF16),
                pltpu.SMEM((edge_count,), jnp.int32),
                pltpu.SMEM((edge_count,), jnp.int32),
                pltpu.SemaphoreType.DMA((4,)),
            ],
        ),
        out_shape=[
            jax.ShapeDtypeStruct((edge_count, width), BF16),
            jax.ShapeDtypeStruct((count, width), BF16),
            jax.ShapeDtypeStruct((HEAD, width), F32),
        ],
        cost_estimate=pl.CostEstimate(
            flops=edge_count * width * width * 6, transcendentals=0, bytes_accessed=16 << 20
        ),
        compiler_params=pltpu.CompilerParams(
            dimension_semantics=("arbitrary",), vmem_limit_bytes=VMEM_LIMIT
        ),
        name="fine",
    )(
        senders * parts, receivers * parts, *operands, edges,
        receivers.reshape(steps, 2, BLK), *extra,
    )


def row_floor(values, divisor):
    return jnp.floor((values + 0.5) * (1.0 / divisor))


def pair_rows(cap):
    return -(-(NCD + cap + 1) // LOW) * LOW


def iota(shape, dim):
    return lax.broadcasted_iota(jnp.int32, shape, dim)


def contract(lhs, rhs, dims):
    return lax.dot_general(lhs, rhs, ((dims[:1], dims[1:]), ((), ())), preferred_element_type=F32)


def prologue_kernel(devices, cap, nodes, send_list, edges, senders, receivers, boundary, parcel, own):
    count, width = edges.shape
    rows = parcel.shape[0] // devices
    high = rows - LOW

    def split(ids):
        owner = row_floor(ids, NCD)
        return owner, ids - owner * NCD

    send_owner, send_local = split(senders[...].astype(F32))
    recv_owner, recv_local = split(receivers[...].astype(F32))
    row_at = iota((count, count), 0)
    col_at = iota((count, count), 1)
    eye = (row_at == col_at).astype(BF16)
    line = iota((LANES, count), 0)

    def columns(items):
        out = jnp.zeros((LANES, count), F32)
        for at, item in enumerate(items):
            out = jnp.where(line == at, item, out)
        return contract(eye, out.astype(BF16), (1, 1))

    cols = columns([send_owner, send_local, recv_owner, recv_local])
    own[...] = cols.astype(BF16)
    owner_col = cols[:, 2:3]
    before = jnp.where((owner_col == recv_owner) & (row_at < col_at), 1.0, 0.0)
    rank = jnp.sum(before, 0, keepdims=True)
    rank_col = columns([rank])[:, :1]
    where_to = recv_owner * high + (NCD - LOW)
    slot = (where_to + rank).astype(jnp.int32)
    place = (where_to + cap).astype(jnp.int32)
    total = devices * high
    at_row = iota((total, count), 0)
    lane = iota((count, LANES), 1).astype(F32)
    here = lane == rank_col
    index_rows = [jnp.where(here, item, 0.0) for item in (cols[:, 0:1], cols[:, 1:2], cols[:, 3:4] + 1.0)]
    index_rows.append(jnp.zeros((count, width - 3 * LANES), F32))
    index_rows = jnp.concatenate(index_rows, 1).astype(BF16)
    sent = dotf((at_row == slot).astype(BF16), edges[...]) + dotf((at_row == place).astype(BF16), index_rows)
    first = nodes[:LOW, :]
    second = nodes[LOW : LOW + high, :].astype(F32)
    second = jnp.where(iota((high, width), 0) < NCD - LOW, second, 0.0)
    for device in range(devices):
        parcel[device * rows : device * rows + LOW, :] = first
        parcel[device * rows + LOW : (device + 1) * rows, :] = (
            sent[device * high : (device + 1) * high, :] + second
        ).astype(BF16)
    ids = send_list[...].astype(F32)
    picks = ids.shape[1]
    upper = row_floor(ids, LANES)
    line = iota((LANES, picks), 0)
    parts = jnp.where(line == 0, upper, jnp.where(line == 1, ids - upper * LANES, 0.0)).astype(BF16)
    same = (iota((picks, picks), 0) == iota((picks, picks), 1)).astype(BF16)
    parts = contract(same, parts, (1, 1))
    chosen = (parts[:, 0:1] * LANES + parts[:, 1:2]).astype(jnp.int32)
    pick = (iota((picks, nodes.shape[0]), 1) == chosen).astype(BF16)
    boundary[...] = dotf(pick, nodes[...]).astype(BF16)


def prologue(devices, cap, nodes, send_list, edges, senders, receivers):
    width = nodes.shape[1]
    args = (nodes, send_list[None, :], edges, senders[None, :], receivers[None, :])
    shapes = [
        (send_list.shape[0], width), (devices * pair_rows(cap), width), (edges.shape[0], LANES)
    ]
    return pl.pallas_call(
        functools.partial(prologue_kernel, devices, cap),
        grid=(1,),
        in_specs=[whole(item.shape) for item in args],
        out_specs=[whole(shape) for shape in shapes],
        out_shape=[jax.ShapeDtypeStruct(shape, BF16) for shape in shapes],
        compiler_params=pltpu.CompilerParams(vmem_limit_bytes=VMEM_LIMIT),
        name="prologue",
    )(*args)


def coarse_kernel(
    devices, cap, parcel, edges, own, nodes, head, w1_far, b1, w2_far, b2, gain, shift,
    nw1_far, nb1, nw2_far, nb2, ngain, nshift, _, new_edges, new_nodes,
    w1, w2, nw1, nw2, sems,
):
    copies = [
        pltpu.make_async_copy(source, target, sems.at[at])
        for at, (source, target) in enumerate(
            ((w1_far, w1), (w2_far, w2), (nw1_far, nw1), (nw2_far, nw2))
        )
    ]
    for copy in copies:
        copy.start()
    width = edges.shape[1]
    total = parcel.shape[0]
    rows = total // devices
    high = rows - LOW

    def messages(edge_rows, send_rows, recv_rows):
        pre = dotf(edge_rows, w1[:width, :]) + dotf(send_rows, w1[width : 2 * width, :])
        pre = pre + dotf(recv_rows, w1[2 * width :, :]) + b1[...]
        hidden = silu_half(0.5 * pre).astype(BF16)
        return norm_rows(dotf(hidden, w2[...]) + b2[...], gain[...], shift[...])

    def lookup(owner, local):
        at = (owner * rows + local).astype(jnp.int32)
        hot = (iota((owner.shape[0], total), 1) == at).astype(BF16)
        return dotf(hot, parcel[...]).astype(BF16)

    tops = jnp.concatenate(
        [parcel[device * rows + LOW : (device + 1) * rows, :] for device in range(devices)], 0
    )
    slots = devices * cap
    column = iota((slots, 1), 0).astype(F32)
    source = row_floor(column, cap)
    rank = column - source * cap
    column_at = iota((slots, devices * high), 1)

    def top_rows(offset):
        at = (source * high + offset).astype(jnp.int32)
        return dotf((column_at == at).astype(BF16), tops)

    edge_rows = top_rows(rank + (NCD - LOW)).astype(BF16)
    index_rows = top_rows(float(NCD - LOW + cap))
    here = iota((slots, LANES), 1).astype(F32) == rank

    def index(part):
        some = index_rows[:, part * LANES : (part + 1) * LANES]
        return jnp.sum(jnp.where(here, some, 0.0), 1, keepdims=True)

    send_rows = lookup(index(0), index(1))
    hot = (iota((slots, LANES), 1) == index(2).astype(jnp.int32) - 1).astype(BF16)
    recv_rows = dotf(hot, nodes[...]).astype(BF16)
    meta = own[...].astype(F32)
    own_send = lookup(meta[:, 0:1], meta[:, 1:2])
    own_recv = lookup(meta[:, 2:3], meta[:, 3:4])
    copies[0].wait()
    copies[1].wait()
    message = messages(
        jnp.concatenate([edge_rows, edges[...]], 0),
        jnp.concatenate([send_rows, own_send], 0),
        jnp.concatenate([recv_rows, own_recv], 0),
    )
    coarse = contract(hot, message[:slots, :].astype(BF16), (0, 0))
    new_edges[...] = (edges[...].astype(F32) + message[slots:, :]).astype(BF16)
    aggregate = (head[...] + coarse[:HEAD, :]).astype(BF16)
    copies[2].wait()
    copies[3].wait()
    new_nodes[...] = node_rows(nodes[:HEAD, :], aggregate, nw1, nb1, nw2, nb2, ngain, nshift)


def coarse_update(devices, cap, parcel, edges, own, nodes, head, weights, node_weights, new_nodes):
    width = nodes.shape[1]
    args = (parcel, edges, own, nodes, head, *weights, *node_weights, new_nodes)
    specs = [whole(item.shape) for item in args]
    specs[3] = whole((LANES, width))
    specs[-1] = pl.BlockSpec(memory_space=pl.ANY)
    specs[0] = pl.BlockSpec(memory_space=pltpu.VMEM)
    far = (5, 7, 11, 13)
    for at in far:
        specs[at] = pl.BlockSpec(memory_space=pl.ANY)
    return pl.pallas_call(
        functools.partial(coarse_kernel, devices, cap),
        grid=(1,),
        in_specs=specs,
        out_specs=[whole(edges.shape), whole((HEAD, width))],
        out_shape=[
            jax.ShapeDtypeStruct(edges.shape, BF16),
            jax.ShapeDtypeStruct(new_nodes.shape, BF16),
        ],
        scratch_shapes=[pltpu.VMEM(args[at].shape, BF16) for at in far]
        + [pltpu.SemaphoreType.DMA((len(far),))],
        input_output_aliases={len(args) - 1: 1},
        compiler_params=pltpu.CompilerParams(vmem_limit_bytes=VMEM_LIMIT),
        name="coarse",
    )(*args)


def shift_ring(count, step):
    return [(item, (item + step) % count) for item in range(count)]


def on_device(
    node_feats, edge_feats, senders, receivers, send_lists, coarse_edges, coarse_senders, coarse_receivers,
    edge_w1, edge_b1, edge_w2, edge_b2, edge_gain, edge_shift,
    node_w1, node_b1, node_w2, node_b2, node_gain, node_shift,
):
    axes = ("gx", "gy")
    devices = lax.axis_size(axes)
    cap = -(-2 * coarse_edges.shape[0] // devices)
    row = lambda vec: vec[None, :]
    weights = (edge_w1, row(edge_b1), edge_w2, row(edge_b2), row(edge_gain), row(edge_shift))
    node_weights = (node_w1, row(node_b1), node_w2, row(node_b2), row(node_gain), row(node_shift))
    boundary, parcel, own = prologue(
        devices, cap, node_feats, send_lists, coarse_edges, coarse_senders, coarse_receivers
    )
    halos = [lax.ppermute(boundary, axis, shift_ring(lax.axis_size(axis), step)) for axis in axes for step in (1, -1)]
    parcel = lax.all_to_all(parcel, axes, 0, 0, tiled=True)
    new_edges, new_nodes, head = fine_update(
        node_feats, halos, edge_feats, senders, receivers, weights, node_weights
    )
    new_coarse, new_nodes = coarse_update(
        devices, cap, parcel, coarse_edges, own, node_feats, head, weights, node_weights, new_nodes
    )
    return new_nodes, new_edges, new_coarse


def solution(mesh):
    split = P(("gx", "gy"), None)
    flat = P(("gx", "gy"))
    placed = (split, split, flat, flat, flat, split, flat, flat) + (P(),) * 12
    return jax.shard_map(
        on_device, mesh=mesh, in_specs=placed, out_specs=(split, split, split), check_vma=False
    )
```

```python
import functools

import jax
import jax.numpy as jnp
from jax import lax
from jax.experimental import pallas as pl
from jax.experimental.pallas import tpu as pltpu
from jax.sharding import PartitionSpec as P


NCD = 20
BLK = 256
WIN = BLK + 16
HEAD = 32
LOW = 16
CHUNK = 64
VMEM_LIMIT = 60 << 20
KEEP_LIMIT = 40 << 20
LANES = 128
F32 = jnp.float32
BF16 = jnp.bfloat16


def dotf(lhs, rhs):
    return jnp.dot(lhs, rhs, preferred_element_type=F32)


def silu_half(half):
    return half + half * jnp.tanh(half)


def norm_rows(values, gain, shift):
    centred = values - jnp.mean(values, -1, keepdims=True)
    variance = jnp.mean(centred * centred, -1, keepdims=True)
    return centred * lax.rsqrt(variance + 1e-05) * gain + shift


def put_rows(table, row, values):
    parts = values.shape[1] // LANES
    for part in range(parts):
        table[pl.ds(row * parts + part, values.shape[0], stride=parts), :] = values[
            :, part * LANES : (part + 1) * LANES
        ]


def node_rows(nodes, aggregate, w1, b1, w2, b2, gain, shift):
    width = nodes.shape[1]
    pre = dotf(nodes, w1[:width, :]) + dotf(aggregate, w1[width:, :]) + b1[...]
    hidden = silu_half(0.5 * pre).astype(BF16)
    return (nodes.astype(F32) + norm_rows(dotf(hidden, w2[...]) + b2[...], gain[...], shift[...])).astype(BF16)


def fine_kernel(
    send_far, recv_far, nodes, halo0, halo1, halo2, halo3, edges, recv_lanes, w1, b1, w2, b2, gain, shift,
    nw1_far, nb1, nw2_far, nb2, ngain, nshift,
    new_edges, new_nodes, head,
    send_table, recv_table, picked_a, picked_b, hidden_a, hidden_b, message_a, message_b, summed, nw1, nw2,
    send4, recv4, sems,
):
    step = pl.program_id(0)
    last = pl.num_programs(0) - 1
    count, width = nodes.shape
    parts = width // LANES
    rows = BLK
    copies = [
        pltpu.make_async_copy(nw1_far, nw1, sems.at[0]),
        pltpu.make_async_copy(nw2_far, nw2, sems.at[1]),
    ]
    index_copies = [
        pltpu.make_async_copy(send_far, send4, sems.at[2]),
        pltpu.make_async_copy(recv_far, recv4, sems.at[3]),
    ]

    def pick(block, out, start, stop):
        base = block * rows
        for row in range(start, stop):
            first = pl.multiple_of(send4[base + row], parts)
            second = pl.multiple_of(recv4[base + row], parts)
            out[row * parts : (row + 1) * parts, :] = (
                send_table[pl.ds(first, parts), :] + recv_table[pl.ds(second, parts), :]
            )

    @pl.when(step == 0)
    def _():
        for copy in index_copies + copies:
            copy.start()
        summed[...] = jnp.zeros_like(summed)
        for start in range(0, count, rows):
            some = nodes[start : start + rows, :]
            put_rows(send_table, start, dotf(some, w1[width : 2 * width, :]))
            put_rows(recv_table, start, dotf(some, w1[2 * width :, :]) + b1[...])
        start = count
        for halo in (halo0, halo1, halo2, halo3):
            put_rows(send_table, start, dotf(halo[...], w1[width : 2 * width, :]))
            start += halo.shape[0]
        for copy in index_copies:
            copy.wait()
        pick(0, picked_a, 0, rows)

    def first_layer(half):
        return dotf(edges[half * rows : (half + 1) * rows, :], w1[:width, :])

    def activate(pre, picked, hidden, start, stop):
        for part in range(parts):
            lanes = slice(part * LANES, (part + 1) * LANES)
            near = picked[pl.ds(start * parts + part, stop - start, stride=parts), :]
            hidden[start:stop, lanes] = silu_half(0.5 * (pre[start:stop, lanes] + near)).astype(BF16)

    def finish(half, out, message, start, stop):
        values = norm_rows(out[start:stop, :] + b2[...], gain[...], shift[...])
        message[start:stop, :] = values.astype(BF16)
        at = slice(half * rows + start, half * rows + stop)
        new_edges[at, :] = (edges[at, :].astype(F32) + values).astype(BF16)

    def collect(half, message):
        first = recv4[(2 * step + half) * rows] // parts
        first = pl.multiple_of((first // 8) * 8, 8)
        ids = recv_lanes[:, half * rows : (half + 1) * rows] - first
        onehot = (lax.broadcasted_iota(jnp.int32, (WIN, rows), 0) == ids).astype(BF16)
        summed[pl.ds(first, WIN), :] += dotf(onehot, message[...])

    chunks = [(start, start + CHUNK) for start in range(0, rows, CHUNK)]
    after = jnp.minimum(2 * step + 2, 2 * last)
    pre_a = first_layer(0)
    for start, stop in chunks:
        activate(pre_a, picked_a, hidden_a, start, stop)
        pick(2 * step + 1, picked_b, start, stop)
    pre_b = first_layer(1)
    out_a = dotf(hidden_a[...], w2[...])
    for start, stop in chunks:
        activate(pre_b, picked_b, hidden_b, start, stop)
        finish(0, out_a, message_a, start, stop)
    out_b = dotf(hidden_b[...], w2[...])
    collect(0, message_a)
    for start, stop in chunks:
        finish(1, out_b, message_b, start, stop)
        pick(after, picked_a, start, stop)
    collect(1, message_b)

    @pl.when(step == last)
    def _():
        for copy in copies:
            copy.wait()
        head[...] = summed[:HEAD, :]
        for start in range(0, count, rows):
            new_nodes[start : start + rows, :] = node_rows(
                nodes[start : start + rows, :], summed[start : start + rows, :].astype(BF16),
                nw1, nb1, nw2, nb2, ngain, nshift,
            )


def whole(shape):
    return pl.BlockSpec(shape, lambda *_: (0,) * len(shape))


def far(item):
    return pltpu.with_memory_space_constraint(item, pltpu.HBM)


def fine_update(nodes, halos, edges, senders, receivers, weights, node_weights):
    count, width = nodes.shape
    edge_count = edges.shape[0]
    parts = width // LANES
    steps = edge_count // (2 * BLK)
    table = count + sum(halo.shape[0] for halo in halos)
    extra = (*weights, *node_weights)
    return pl.pallas_call(
        fine_kernel,
        grid_spec=pltpu.PrefetchScalarGridSpec(
            num_scalar_prefetch=0,
            grid=(steps,),
            in_specs=[pl.BlockSpec(memory_space=pl.ANY)] * 2
            + [whole(nodes.shape)] + [pl.BlockSpec(memory_space=pltpu.VMEM)] * len(halos)
            + [
                pl.BlockSpec((2 * BLK, width), lambda i, *_: (i, 0)),
                pl.BlockSpec((1, 2 * BLK), lambda i, *_: (0, i)),
            ]
            + [
                pl.BlockSpec(memory_space=pl.ANY) if at in (6, 8) else whole(item.shape)
                for at, item in enumerate(extra)
            ],
            out_specs=[
                pl.BlockSpec((2 * BLK, width), lambda i, *_: (i, 0)),
                whole((count, width)),
                whole((HEAD, width)),
            ],
            scratch_shapes=[
                pltpu.VMEM((table * parts, LANES), F32),
                pltpu.VMEM((count * parts, LANES), F32),
                pltpu.VMEM((BLK * parts, LANES), F32),
                pltpu.VMEM((BLK * parts, LANES), F32),
            ]
            + [pltpu.VMEM((BLK, width), BF16)] * 4
            + [
                pltpu.VMEM((count + WIN, width), F32),
                pltpu.VMEM(node_weights[0].shape, BF16),
                pltpu.VMEM(node_weights[2].shape, BF16),
                pltpu.SMEM((edge_count,), jnp.int32),
                pltpu.SMEM((edge_count,), jnp.int32),
                pltpu.SemaphoreType.DMA((4,)),
            ],
        ),
        out_shape=[
            jax.ShapeDtypeStruct((edge_count, width), BF16),
            jax.ShapeDtypeStruct((count, width), BF16),
            jax.ShapeDtypeStruct((HEAD, width), F32),
        ],
        cost_estimate=pl.CostEstimate(
            flops=edge_count * width * width * 6, transcendentals=0, bytes_accessed=16 << 20
        ),
        compiler_params=pltpu.CompilerParams(
            dimension_semantics=("arbitrary",), vmem_limit_bytes=KEEP_LIMIT
        ),
        name="fine",
    )(
        far(senders * parts), far(receivers * parts), far(nodes), *halos, far(edges),
        far(receivers[None, :]), *map(far, extra),
    )


def row_floor(values, divisor):
    return jnp.floor((values + 0.5) * (1.0 / divisor))


def pair_rows(cap):
    return -(-(NCD + cap + 1) // LOW) * LOW


def iota(shape, dim):
    return lax.broadcasted_iota(jnp.int32, shape, dim)


def contract(lhs, rhs, dims):
    return lax.dot_general(lhs, rhs, ((dims[:1], dims[1:]), ((), ())), preferred_element_type=F32)


def prologue_kernel(
    devices, cap, first_nodes, nodes_far, send_list, edges, senders, receivers, boundary, parcel, own, nodes, sem
):
    copy = pltpu.make_async_copy(nodes_far, nodes, sem)
    copy.start()
    count, width = edges.shape
    rows = parcel.shape[0] // devices
    high = rows - LOW

    def split(ids):
        owner = row_floor(ids, NCD)
        return owner, ids - owner * NCD

    send_owner, send_local = split(senders[...].astype(F32))
    recv_owner, recv_local = split(receivers[...].astype(F32))
    row_at = iota((count, count), 0)
    col_at = iota((count, count), 1)
    eye = (row_at == col_at).astype(BF16)
    line = iota((LANES, count), 0)

    def columns(items):
        out = jnp.zeros((LANES, count), F32)
        for at, item in enumerate(items):
            out = jnp.where(line == at, item, out)
        return contract(eye, out.astype(BF16), (1, 1))

    cols = columns([send_owner, send_local, recv_owner, recv_local])
    own[...] = cols.astype(BF16)
    owner_col = cols[:, 2:3]
    before = jnp.where((owner_col == recv_owner) & (row_at < col_at), 1.0, 0.0)
    rank = jnp.sum(before, 0, keepdims=True)
    rank_col = columns([rank])[:, :1]
    where_to = recv_owner * high + (NCD - LOW)
    slot = (where_to + rank).astype(jnp.int32)
    place = (where_to + cap).astype(jnp.int32)
    total = devices * high
    at_row = iota((total, count), 0)
    lane = iota((count, LANES), 1).astype(F32)
    here = lane == rank_col
    index_rows = [jnp.where(here, item, 0.0) for item in (cols[:, 0:1], cols[:, 1:2], cols[:, 3:4] + 1.0)]
    index_rows.append(jnp.zeros((count, width - 3 * LANES), F32))
    index_rows = jnp.concatenate(index_rows, 1).astype(BF16)
    sent = dotf((at_row == slot).astype(BF16), edges[...]) + dotf((at_row == place).astype(BF16), index_rows)
    first = first_nodes[:LOW, :]
    second = first_nodes[LOW : LOW + high, :].astype(F32)
    second = jnp.where(iota((high, width), 0) < NCD - LOW, second, 0.0)
    for device in range(devices):
        parcel[device * rows : device * rows + LOW, :] = first
        parcel[device * rows + LOW : (device + 1) * rows, :] = (
            sent[device * high : (device + 1) * high, :] + second
        ).astype(BF16)
    ids = send_list[...].astype(F32)
    picks = ids.shape[1]
    upper = row_floor(ids, LANES)
    line = iota((LANES, picks), 0)
    parts = jnp.where(line == 0, upper, jnp.where(line == 1, ids - upper * LANES, 0.0)).astype(BF16)
    same = (iota((picks, picks), 0) == iota((picks, picks), 1)).astype(BF16)
    parts = contract(same, parts, (1, 1))
    chosen = (parts[:, 0:1] * LANES + parts[:, 1:2]).astype(jnp.int32)
    pick = (iota((picks, nodes.shape[0]), 1) == chosen).astype(BF16)
    copy.wait()
    boundary[...] = dotf(pick, nodes[...]).astype(BF16)


def prologue(devices, cap, nodes, send_list, edges, senders, receivers):
    width = nodes.shape[1]
    args = (nodes, nodes, send_list[None, :], edges, senders[None, :], receivers[None, :])
    specs = [whole(item.shape) for item in args]
    specs[0] = whole((pair_rows(cap), width))
    specs[1] = pl.BlockSpec(memory_space=pl.ANY)
    shapes = [
        (send_list.shape[0], width), (devices * pair_rows(cap), width), (edges.shape[0], LANES)
    ]
    return pl.pallas_call(
        functools.partial(prologue_kernel, devices, cap),
        grid=(1,),
        in_specs=specs,
        out_specs=[whole(shape) for shape in shapes],
        scratch_shapes=[pltpu.VMEM(nodes.shape, BF16), pltpu.SemaphoreType.DMA],
        out_shape=[jax.ShapeDtypeStruct(shape, BF16) for shape in shapes],
        compiler_params=pltpu.CompilerParams(vmem_limit_bytes=VMEM_LIMIT),
        name="prologue",
    )(*args)


def coarse_kernel(
    devices, cap, parcel, edges, own, nodes, head, w1_far, b1, w2_far, b2, gain, shift,
    nw1_far, nb1, nw2_far, nb2, ngain, nshift, _, new_edges, new_nodes,
    w1, w2, nw1, nw2, sems,
):
    copies = [
        pltpu.make_async_copy(source, target, sems.at[at])
        for at, (source, target) in enumerate(
            ((w1_far, w1), (w2_far, w2), (nw1_far, nw1), (nw2_far, nw2))
        )
    ]
    for copy in copies:
        copy.start()
    width = edges.shape[1]
    total = parcel.shape[0]
    rows = total // devices
    high = rows - LOW

    def messages(edge_rows, send_rows, recv_rows):
        pre = dotf(edge_rows, w1[:width, :]) + dotf(send_rows, w1[width : 2 * width, :])
        pre = pre + dotf(recv_rows, w1[2 * width :, :]) + b1[...]
        hidden = silu_half(0.5 * pre).astype(BF16)
        return norm_rows(dotf(hidden, w2[...]) + b2[...], gain[...], shift[...])

    def lookup(owner, local):
        at = (owner * rows + local).astype(jnp.int32)
        hot = (iota((owner.shape[0], total), 1) == at).astype(BF16)
        return dotf(hot, parcel[...]).astype(BF16)

    tops = jnp.concatenate(
        [parcel[device * rows + LOW : (device + 1) * rows, :] for device in range(devices)], 0
    )
    slots = devices * cap
    column = iota((slots, 1), 0).astype(F32)
    source = row_floor(column, cap)
    rank = column - source * cap
    column_at = iota((slots, devices * high), 1)

    def top_rows(offset):
        at = (source * high + offset).astype(jnp.int32)
        return dotf((column_at == at).astype(BF16), tops)

    edge_rows = top_rows(rank + (NCD - LOW)).astype(BF16)
    index_rows = top_rows(float(NCD - LOW + cap))
    here = iota((slots, LANES), 1).astype(F32) == rank

    def index(part):
        some = index_rows[:, part * LANES : (part + 1) * LANES]
        return jnp.sum(jnp.where(here, some, 0.0), 1, keepdims=True)

    send_rows = lookup(index(0), index(1))
    hot = (iota((slots, LANES), 1) == index(2).astype(jnp.int32) - 1).astype(BF16)
    recv_rows = dotf(hot, nodes[...]).astype(BF16)
    meta = own[...].astype(F32)
    own_send = lookup(meta[:, 0:1], meta[:, 1:2])
    own_recv = lookup(meta[:, 2:3], meta[:, 3:4])
    copies[0].wait()
    copies[1].wait()
    message = messages(
        jnp.concatenate([edge_rows, edges[...]], 0),
        jnp.concatenate([send_rows, own_send], 0),
        jnp.concatenate([recv_rows, own_recv], 0),
    )
    coarse = contract(hot, message[:slots, :].astype(BF16), (0, 0))
    new_edges[...] = (edges[...].astype(F32) + message[slots:, :]).astype(BF16)
    aggregate = (head[...] + coarse[:HEAD, :]).astype(BF16)
    copies[2].wait()
    copies[3].wait()
    new_nodes[...] = node_rows(nodes[:HEAD, :], aggregate, nw1, nb1, nw2, nb2, ngain, nshift)


def coarse_update(devices, cap, parcel, edges, own, nodes, head, weights, node_weights, new_nodes):
    width = nodes.shape[1]
    args = (parcel, edges, own, nodes, head, *weights, *node_weights, new_nodes)
    specs = [whole(item.shape) for item in args]
    near = (0, 4)
    args = tuple(item if at in near else far(item) for at, item in enumerate(args))
    specs[3] = whole((LANES, width))
    specs[-1] = pl.BlockSpec(memory_space=pl.ANY)
    for at in near:
        specs[at] = pl.BlockSpec(memory_space=pltpu.VMEM)
    late = (5, 7, 11, 13)
    for at in late:
        specs[at] = pl.BlockSpec(memory_space=pl.ANY)
    return pl.pallas_call(
        functools.partial(coarse_kernel, devices, cap),
        grid=(1,),
        in_specs=specs,
        out_specs=[whole(edges.shape), whole((HEAD, width))],
        out_shape=[
            jax.ShapeDtypeStruct(edges.shape, BF16),
            jax.ShapeDtypeStruct(new_nodes.shape, BF16),
        ],
        scratch_shapes=[pltpu.VMEM(args[at].shape, BF16) for at in late]
        + [pltpu.SemaphoreType.DMA((len(late),))],
        input_output_aliases={len(args) - 1: 1},
        compiler_params=pltpu.CompilerParams(vmem_limit_bytes=KEEP_LIMIT),
        name="coarse",
    )(*args)


def shift_ring(count, step):
    return [(item, (item + step) % count) for item in range(count)]


def on_device(
    node_feats, edge_feats, senders, receivers, send_lists, coarse_edges, coarse_senders, coarse_receivers,
    edge_w1, edge_b1, edge_w2, edge_b2, edge_gain, edge_shift,
    node_w1, node_b1, node_w2, node_b2, node_gain, node_shift,
):
    axes = ("gx", "gy")
    devices = lax.axis_size(axes)
    cap = -(-2 * coarse_edges.shape[0] // devices)
    row = lambda vec: vec[None, :]
    weights = (edge_w1, row(edge_b1), edge_w2, row(edge_b2), row(edge_gain), row(edge_shift))
    node_weights = (node_w1, row(node_b1), node_w2, row(node_b2), row(node_gain), row(node_shift))
    boundary, parcel, own = prologue(
        devices, cap, node_feats, send_lists, coarse_edges, coarse_senders, coarse_receivers
    )
    halos = [
        lax.ppermute(boundary, axis, shift_ring(lax.axis_size(axis), step))
        for axis in axes
        for step in (1, -1)
    ]
    parcel = lax.all_to_all(parcel, axes, 0, 0, tiled=True)
    new_edges, new_nodes, head = fine_update(
        node_feats, halos, edge_feats, senders, receivers, weights, node_weights
    )
    new_coarse, new_nodes = coarse_update(
        devices, cap, parcel, coarse_edges, own, node_feats, head, weights, node_weights, new_nodes
    )
    return new_nodes, new_edges, new_coarse


def solution(mesh):
    split = P(("gx", "gy"), None)
    flat = P(("gx", "gy"))
    placed = (split, split, flat, flat, flat, split, flat, flat) + (P(),) * 12
    return jax.shard_map(
        on_device, mesh=mesh, in_specs=placed, out_specs=(split, split, split), check_vma=False
    )
```

```python
import functools

import jax
import jax.numpy as jnp
from jax import lax
from jax.experimental import pallas as pl
from jax.experimental.pallas import tpu as pltpu
from jax.sharding import PartitionSpec as P


NCD = 20
BLK = 256
WIN = BLK + 16
HEAD = 32
LOW = 16
CHUNK = 64
VMEM_LIMIT = 60 << 20
KEEP_LIMIT = 40 << 20
LANES = 128
F32 = jnp.float32
BF16 = jnp.bfloat16


def dotf(lhs, rhs):
    return jnp.dot(lhs, rhs, preferred_element_type=F32)


def silu_half(half):
    return half + half * jnp.tanh(half)


def norm_rows(values, gain, shift):
    centred = values - jnp.mean(values, -1, keepdims=True)
    variance = jnp.mean(centred * centred, -1, keepdims=True)
    return centred * lax.rsqrt(variance + 1e-05) * gain + shift


def put_rows(table, row, values):
    parts = values.shape[1] // LANES
    for part in range(parts):
        table[pl.ds(row * parts + part, values.shape[0], stride=parts), :] = values[
            :, part * LANES : (part + 1) * LANES
        ]


def node_rows(nodes, aggregate, w1, b1, w2, b2, gain, shift):
    width = nodes.shape[1]
    pre = dotf(nodes, w1[:width, :]) + dotf(aggregate, w1[width:, :]) + b1[...]
    hidden = silu_half(0.5 * pre).astype(BF16)
    return (nodes.astype(F32) + norm_rows(dotf(hidden, w2[...]) + b2[...], gain[...], shift[...])).astype(BF16)


def fine_kernel(
    carried, send_far, recv_far, nodes, halo0, halo1, halo2, halo3, edges, recv_lanes, w1, b1, w2, b2, gain, shift,
    nb1, nb2, ngain, nshift, *refs,
):
    sources, refs = refs[:carried], refs[carried:]
    new_edges, new_nodes, head = refs[:3]
    targets, refs = refs[3 : 3 + carried], refs[3 + carried :]
    send_table, recv_table, picked_a, picked_b, hidden_a, hidden_b, message_a, message_b, summed = refs[:9]
    send4, recv4, sems = refs[9:]
    nw1, nw2 = targets[:2]
    step = pl.program_id(0)
    last = pl.num_programs(0) - 1
    count, width = nodes.shape
    parts = width // LANES
    rows = BLK
    copies = [
        pltpu.make_async_copy(source.at[pl.ds(0, target.shape[0]), :], target, sems.at[2 + at])
        for at, (source, target) in enumerate(zip(sources, targets))
    ]
    index_copies = [
        pltpu.make_async_copy(send_far, send4, sems.at[0]),
        pltpu.make_async_copy(recv_far, recv4, sems.at[1]),
    ]

    def pick(block, out, start, stop):
        base = block * rows
        for row in range(start, stop):
            first = pl.multiple_of(send4[base + row], parts)
            second = pl.multiple_of(recv4[base + row], parts)
            out[row * parts : (row + 1) * parts, :] = (
                send_table[pl.ds(first, parts), :] + recv_table[pl.ds(second, parts), :]
            )

    @pl.when(step == 0)
    def _():
        for copy in index_copies + copies:
            copy.start()
        summed[...] = jnp.zeros_like(summed)
        for start in range(0, count, rows):
            some = nodes[start : start + rows, :]
            put_rows(send_table, start, dotf(some, w1[width : 2 * width, :]))
            put_rows(recv_table, start, dotf(some, w1[2 * width :, :]) + b1[...])
        start = count
        for halo in (halo0, halo1, halo2, halo3):
            put_rows(send_table, start, dotf(halo[...], w1[width : 2 * width, :]))
            start += halo.shape[0]
        for copy in index_copies:
            copy.wait()
        pick(0, picked_a, 0, rows)

    def first_layer(half):
        return dotf(edges[half * rows : (half + 1) * rows, :], w1[:width, :])

    def activate(pre, picked, hidden, start, stop):
        for part in range(parts):
            lanes = slice(part * LANES, (part + 1) * LANES)
            near = picked[pl.ds(start * parts + part, stop - start, stride=parts), :]
            hidden[start:stop, lanes] = silu_half(0.5 * (pre[start:stop, lanes] + near)).astype(BF16)

    def finish(half, out, message, start, stop):
        values = norm_rows(out[start:stop, :] + b2[...], gain[...], shift[...])
        message[start:stop, :] = values.astype(BF16)
        at = slice(half * rows + start, half * rows + stop)
        new_edges[at, :] = (edges[at, :].astype(F32) + values).astype(BF16)

    def collect(half, message):
        first = recv4[(2 * step + half) * rows] // parts
        first = pl.multiple_of((first // 8) * 8, 8)
        ids = recv_lanes[:, half * rows : (half + 1) * rows] - first
        onehot = (lax.broadcasted_iota(jnp.int32, (WIN, rows), 0) == ids).astype(BF16)
        summed[pl.ds(first, WIN), :] += dotf(onehot, message[...])

    chunks = [(start, start + CHUNK) for start in range(0, rows, CHUNK)]
    after = jnp.minimum(2 * step + 2, 2 * last)
    pre_a = first_layer(0)
    for start, stop in chunks:
        activate(pre_a, picked_a, hidden_a, start, stop)
        pick(2 * step + 1, picked_b, start, stop)
    pre_b = first_layer(1)
    out_a = dotf(hidden_a[...], w2[...])
    for start, stop in chunks:
        activate(pre_b, picked_b, hidden_b, start, stop)
        finish(0, out_a, message_a, start, stop)
    out_b = dotf(hidden_b[...], w2[...])
    collect(0, message_a)
    for start, stop in chunks:
        finish(1, out_b, message_b, start, stop)
        pick(after, picked_a, start, stop)
    collect(1, message_b)

    @pl.when(step == last)
    def _():
        for copy in copies:
            copy.wait()
        head[...] = summed[:HEAD, :]
        for start in range(0, count, rows):
            new_nodes[start : start + rows, :] = node_rows(
                nodes[start : start + rows, :], summed[start : start + rows, :].astype(BF16),
                nw1, nb1, nw2, nb2, ngain, nshift,
            )


def whole(shape):
    return pl.BlockSpec(shape, lambda *_: (0,) * len(shape))


def far(item):
    return pltpu.with_memory_space_constraint(item, pltpu.HBM)


def fine_update(nodes, halos, edges, senders, receivers, weights, node_weights, carry):
    count, width = nodes.shape
    edge_count = edges.shape[0]
    parts = width // LANES
    steps = edge_count // (2 * BLK)
    table = count + sum(halo.shape[0] for halo in halos)
    extra = (*weights, *(node_weights[at] for at in (1, 3, 4, 5)))
    items = [item for item, _ in carry]
    kept = [jax.ShapeDtypeStruct((rows, item.shape[1]), item.dtype) for item, rows in carry]
    return pl.pallas_call(
        functools.partial(fine_kernel, len(carry)),
        grid_spec=pltpu.PrefetchScalarGridSpec(
            num_scalar_prefetch=0,
            grid=(steps,),
            in_specs=[pl.BlockSpec(memory_space=pl.ANY)] * 2
            + [whole(nodes.shape)] + [whole(halo.shape) for halo in halos]
            + [
                pl.BlockSpec((2 * BLK, width), lambda i, *_: (i, 0)),
                pl.BlockSpec((1, 2 * BLK), lambda i, *_: (0, i)),
            ]
            + [whole(item.shape) for item in extra]
            + [pl.BlockSpec(memory_space=pl.ANY)] * len(carry),
            out_specs=[
                pl.BlockSpec((2 * BLK, width), lambda i, *_: (i, 0)),
                whole((count, width)),
                whole((HEAD, width)),
            ]
            + [pl.BlockSpec(memory_space=pltpu.VMEM)] * len(carry),
            scratch_shapes=[
                pltpu.VMEM((table * parts, LANES), F32),
                pltpu.VMEM((count * parts, LANES), F32),
                pltpu.VMEM((BLK * parts, LANES), F32),
                pltpu.VMEM((BLK * parts, LANES), F32),
            ]
            + [pltpu.VMEM((BLK, width), BF16)] * 4
            + [
                pltpu.VMEM((count + WIN, width), F32),
                pltpu.SMEM((edge_count,), jnp.int32),
                pltpu.SMEM((edge_count,), jnp.int32),
                pltpu.SemaphoreType.DMA((2 + len(carry),)),
            ],
        ),
        out_shape=[
            jax.ShapeDtypeStruct((edge_count, width), BF16),
            jax.ShapeDtypeStruct((count, width), BF16),
            jax.ShapeDtypeStruct((HEAD, width), F32),
        ]
        + kept,
        cost_estimate=pl.CostEstimate(
            flops=edge_count * width * width * 6, transcendentals=0, bytes_accessed=16 << 20
        ),
        compiler_params=pltpu.CompilerParams(
            dimension_semantics=("arbitrary",), vmem_limit_bytes=KEEP_LIMIT
        ),
        name="fine",
    )(
        far(senders * parts), far(receivers * parts), far(nodes), *map(far, halos), far(edges),
        far(receivers[None, :]), *map(far, extra), *map(far, items),
    )


def row_floor(values, divisor):
    return jnp.floor((values + 0.5) * (1.0 / divisor))


def pair_rows(cap):
    return -(-(NCD + cap + 1) // LOW) * LOW


def iota(shape, dim):
    return lax.broadcasted_iota(jnp.int32, shape, dim)


def contract(lhs, rhs, dims):
    return lax.dot_general(lhs, rhs, ((dims[:1], dims[1:]), ((), ())), preferred_element_type=F32)


def prologue_kernel(
    devices, cap, first_nodes, nodes_far, send_list, edges, senders, receivers, boundary, parcel, own, nodes, sem
):
    copy = pltpu.make_async_copy(nodes_far, nodes, sem)
    copy.start()
    count, width = edges.shape
    rows = parcel.shape[0] // devices
    high = rows - LOW

    def split(ids):
        owner = row_floor(ids, NCD)
        return owner, ids - owner * NCD

    send_owner, send_local = split(senders[...].astype(F32))
    recv_owner, recv_local = split(receivers[...].astype(F32))
    row_at = iota((count, count), 0)
    col_at = iota((count, count), 1)
    eye = (row_at == col_at).astype(BF16)
    line = iota((LANES, count), 0)

    def columns(items):
        out = jnp.zeros((LANES, count), F32)
        for at, item in enumerate(items):
            out = jnp.where(line == at, item, out)
        return contract(eye, out.astype(BF16), (1, 1))

    cols = columns([send_owner, send_local, recv_owner, recv_local])
    own[...] = cols.astype(BF16)
    owner_col = cols[:, 2:3]
    before = jnp.where((owner_col == recv_owner) & (row_at < col_at), 1.0, 0.0)
    rank = jnp.sum(before, 0, keepdims=True)
    rank_col = columns([rank])[:, :1]
    where_to = recv_owner * high + (NCD - LOW)
    slot = (where_to + rank).astype(jnp.int32)
    place = (where_to + cap).astype(jnp.int32)
    total = devices * high
    at_row = iota((total, count), 0)
    lane = iota((count, LANES), 1).astype(F32)
    here = lane == rank_col
    index_rows = [jnp.where(here, item, 0.0) for item in (cols[:, 0:1], cols[:, 1:2], cols[:, 3:4] + 1.0)]
    index_rows.append(jnp.zeros((count, width - 3 * LANES), F32))
    index_rows = jnp.concatenate(index_rows, 1).astype(BF16)
    sent = dotf((at_row == slot).astype(BF16), edges[...]) + dotf((at_row == place).astype(BF16), index_rows)
    first = first_nodes[:LOW, :]
    second = first_nodes[LOW : LOW + high, :].astype(F32)
    second = jnp.where(iota((high, width), 0) < NCD - LOW, second, 0.0)
    for device in range(devices):
        parcel[device * rows : device * rows + LOW, :] = first
        parcel[device * rows + LOW : (device + 1) * rows, :] = (
            sent[device * high : (device + 1) * high, :] + second
        ).astype(BF16)
    ids = send_list[...].astype(F32)
    picks = ids.shape[1]
    upper = row_floor(ids, LANES)
    line = iota((LANES, picks), 0)
    parts = jnp.where(line == 0, upper, jnp.where(line == 1, ids - upper * LANES, 0.0)).astype(BF16)
    same = (iota((picks, picks), 0) == iota((picks, picks), 1)).astype(BF16)
    parts = contract(same, parts, (1, 1))
    chosen = (parts[:, 0:1] * LANES + parts[:, 1:2]).astype(jnp.int32)
    pick = (iota((picks, nodes.shape[0]), 1) == chosen).astype(BF16)
    copy.wait()
    boundary[...] = dotf(pick, nodes[...]).astype(BF16)


def prologue(devices, cap, nodes, send_list, edges, senders, receivers):
    width = nodes.shape[1]
    args = (nodes, nodes, send_list[None, :], edges, senders[None, :], receivers[None, :])
    specs = [whole(item.shape) for item in args]
    specs[0] = whole((pair_rows(cap), width))
    specs[1] = pl.BlockSpec(memory_space=pl.ANY)
    shapes = [
        (send_list.shape[0], width), (devices * pair_rows(cap), width), (edges.shape[0], LANES)
    ]
    return pl.pallas_call(
        functools.partial(prologue_kernel, devices, cap),
        grid=(1,),
        in_specs=specs,
        out_specs=[whole(shape) for shape in shapes],
        scratch_shapes=[pltpu.VMEM(nodes.shape, BF16), pltpu.SemaphoreType.DMA],
        out_shape=[jax.ShapeDtypeStruct(shape, BF16) for shape in shapes],
        compiler_params=pltpu.CompilerParams(vmem_limit_bytes=VMEM_LIMIT),
        name="prologue",
    )(*args)


def coarse_kernel(
    devices, cap, parcel, edges, own, nodes, head, w1, b1, w2, b2, gain, shift,
    nw1, nb1, nw2, nb2, ngain, nshift, _, new_edges, new_nodes,
):
    width = edges.shape[1]
    total = parcel.shape[0]
    rows = total // devices
    high = rows - LOW

    def messages(edge_rows, send_rows, recv_rows):
        pre = dotf(edge_rows, w1[:width, :]) + dotf(send_rows, w1[width : 2 * width, :])
        pre = pre + dotf(recv_rows, w1[2 * width :, :]) + b1[...]
        hidden = silu_half(0.5 * pre).astype(BF16)
        return norm_rows(dotf(hidden, w2[...]) + b2[...], gain[...], shift[...])

    def lookup(owner, local):
        at = (owner * rows + local).astype(jnp.int32)
        hot = (iota((owner.shape[0], total), 1) == at).astype(BF16)
        return dotf(hot, parcel[...]).astype(BF16)

    tops = jnp.concatenate(
        [parcel[device * rows + LOW : (device + 1) * rows, :] for device in range(devices)], 0
    )
    slots = devices * cap
    column = iota((slots, 1), 0).astype(F32)
    source = row_floor(column, cap)
    rank = column - source * cap
    column_at = iota((slots, devices * high), 1)

    def top_rows(offset):
        at = (source * high + offset).astype(jnp.int32)
        return dotf((column_at == at).astype(BF16), tops)

    edge_rows = top_rows(rank + (NCD - LOW)).astype(BF16)
    index_rows = top_rows(float(NCD - LOW + cap))
    here = iota((slots, LANES), 1).astype(F32) == rank

    def index(part):
        some = index_rows[:, part * LANES : (part + 1) * LANES]
        return jnp.sum(jnp.where(here, some, 0.0), 1, keepdims=True)

    send_rows = lookup(index(0), index(1))
    hot = (iota((slots, LANES), 1) == index(2).astype(jnp.int32) - 1).astype(BF16)
    recv_rows = dotf(hot, nodes[...]).astype(BF16)
    meta = own[...].astype(F32)
    own_send = lookup(meta[:, 0:1], meta[:, 1:2])
    own_recv = lookup(meta[:, 2:3], meta[:, 3:4])
    message = messages(
        jnp.concatenate([edge_rows, edges[...]], 0),
        jnp.concatenate([send_rows, own_send], 0),
        jnp.concatenate([recv_rows, own_recv], 0),
    )
    coarse = contract(hot, message[:slots, :].astype(BF16), (0, 0))
    new_edges[...] = (edges[...].astype(F32) + message[slots:, :]).astype(BF16)
    aggregate = (head[...] + coarse[:HEAD, :]).astype(BF16)
    new_nodes[...] = node_rows(nodes[:HEAD, :], aggregate, nw1, nb1, nw2, nb2, ngain, nshift)


def coarse_update(devices, cap, parcel, edges, own, nodes, head, weights, node_weights, new_nodes):
    width = nodes.shape[1]
    args = (parcel, edges, own, nodes, head, *weights, *node_weights, new_nodes)
    near = (0, 1, 2, 3, 4, 5, 7)
    args = tuple(item if at in near else far(item) for at, item in enumerate(args))
    specs = [
        pl.BlockSpec(memory_space=pltpu.VMEM) if at in near else whole(item.shape)
        for at, item in enumerate(args)
    ]
    specs[-1] = pl.BlockSpec(memory_space=pl.ANY)
    return pl.pallas_call(
        functools.partial(coarse_kernel, devices, cap),
        grid=(1,),
        in_specs=specs,
        out_specs=[whole(edges.shape), whole((HEAD, width))],
        out_shape=[
            jax.ShapeDtypeStruct(edges.shape, BF16),
            jax.ShapeDtypeStruct(new_nodes.shape, BF16),
        ],
        input_output_aliases={len(args) - 1: 1},
        compiler_params=pltpu.CompilerParams(vmem_limit_bytes=KEEP_LIMIT),
        name="coarse",
    )(*args)


def shift_ring(count, step):
    return [(item, (item + step) % count) for item in range(count)]


def on_device(
    node_feats, edge_feats, senders, receivers, send_lists, coarse_edges, coarse_senders, coarse_receivers,
    edge_w1, edge_b1, edge_w2, edge_b2, edge_gain, edge_shift,
    node_w1, node_b1, node_w2, node_b2, node_gain, node_shift,
):
    axes = ("gx", "gy")
    devices = lax.axis_size(axes)
    cap = -(-2 * coarse_edges.shape[0] // devices)
    row = lambda vec: vec[None, :]
    weights = (edge_w1, row(edge_b1), edge_w2, row(edge_b2), row(edge_gain), row(edge_shift))
    node_weights = (node_w1, row(node_b1), node_w2, row(node_b2), row(node_gain), row(node_shift))
    boundary, parcel, own = prologue(
        devices, cap, node_feats, send_lists, coarse_edges, coarse_senders, coarse_receivers
    )
    halos = [lax.ppermute(boundary, axis, shift_ring(lax.axis_size(axis), step)) for axis in axes for step in (1, -1)]
    parcel = lax.all_to_all(parcel, axes, 0, 0, tiled=True)
    late = (node_weights[0], node_weights[2], coarse_edges, own, node_feats, edge_w1, edge_w2)
    carry = [(item, LANES if item is node_feats else item.shape[0]) for item in late]
    new_edges, new_nodes, head, *kept = fine_update(
        node_feats, halos, edge_feats, senders, receivers, weights, node_weights, carry
    )
    weights = (kept[5], weights[1], kept[6], *weights[3:])
    new_coarse, new_nodes = coarse_update(
        devices, cap, parcel, kept[2], kept[3], kept[4], head, weights, node_weights, new_nodes
    )
    return new_nodes, new_edges, new_coarse


def solution(mesh):
    split = P(("gx", "gy"), None)
    flat = P(("gx", "gy"))
    placed = (split, split, flat, flat, flat, split, flat, flat) + (P(),) * 12
    return jax.shard_map(
        on_device, mesh=mesh, in_specs=placed, out_specs=(split, split, split), check_vma=False
    )
```
